16 devices in a mesh: dp: 4 (over z, y), ep: 4 (over x, core).
Axes of the slice: x: 2, y: 2, z: 2, core: 2. Of those that a mesh axis runs over, the one named last changes fastest.
Arguments:
- grad_y: bfloat16 [1024, 1024], P(('dp', 'ep')), parts along dimension 0
- gate_vals: float32 [1024, 8], P(('dp', 'ep')), parts along dimension 0
- topk_idx: int32 [1024, 8], P(('dp', 'ep')), parts along dimension 0
- slot_ids: int32 [1024, 8], P(('dp', 'ep')), parts along dimension 0
- pair_counts: int32 [16, 32], P(('dp', 'ep')), parts along dimension 0
- y_routed: bfloat16 [1024, 8, 1024], P(('dp', 'ep')), parts along dimension 0
- x_disp: bfloat16 [128, 128, 1024], P(('dp', 'ep')), parts along dimension 0
- h_gate: bfloat16 [128, 128, 512], P(('dp', 'ep')), parts along dimension 0
- h_up: bfloat16 [128, 128, 512], P(('dp', 'ep')), parts along dimension 0
- w_gate: bfloat16 [32, 1024, 512], P('ep')
- w_up: bfloat16 [32, 1024, 512], P('ep')
- w_down: bfloat16 [32, 512, 1024], P('ep')
Outputs:
- output 1: bfloat16 [1024, 1024], P(('dp', 'ep')), parts along dimension 0
- output 2: float32 [1024, 8], P(('dp', 'ep')), parts along dimension 0
- output 3: float32 [128, 1024, 512], P(('dp', 'ep')), parts along dimension 0
- output 4: float32 [128, 1024, 512], P(('dp', 'ep')), parts along dimension 0
- output 5: float32 [128, 512, 1024], P(('dp', 'ep')), parts along dimension 0
There are 4 independent parts. The reference program is written for one: setup_inputs(seed, part) draws one part's arguments, and reference() takes and returns one part's arrays. A program takes and returns all parts, laid end to end along the dimension named above; an argument that names none is the same for every part.
All inputs are finite; a program needn't handle non-finite values.
Results may differ from the reference program's by a relative error of at most 0.0149207.
Values are sent between devices in bfloat16 or wider.
A program may use at most 1 GiB of HBM per device.

```python
import jax
import jax.numpy as jnp
from jax import lax

GROUP_DEV = 4
TOKENS_DEV = 64
EXPERTS = 32
TOP_K = 8
MODEL_DIM = 1024
FFN_DIM = 512
CAPACITY = 32
N_TOKENS = GROUP_DEV * TOKENS_DEV
EXPERT_ROWS = GROUP_DEV * CAPACITY


def setup_inputs(seed: int = 0, part: int = 0) -> dict:
    base_key = jax.random.fold_in(jax.random.key(seed), part)
    key_list = jax.random.split(base_key, 8)
    weight_keys = jax.random.split(jax.random.key(seed + 1), 3)
    key_noise, key_bias, key_hot = jax.random.split(key_list[0], 3)
    expert_iota = jnp.arange(EXPERTS, dtype=jnp.int32)
    token_iota = jnp.arange(TOKENS_DEV, dtype=jnp.int32)
    noise_int = jax.random.randint(key_noise, (GROUP_DEV, TOKENS_DEV, EXPERTS), 0, 4 * EXPERTS)
    bias_base = jax.random.randint(key_bias, (EXPERTS,), 0, 2 * EXPERTS)
    bias_int = (bias_base * bias_base) // (4 * EXPERTS)
    hot_expert = jax.random.randint(key_hot, (GROUP_DEV,), 0, EXPERTS)
    hot_bonus = jnp.where((token_iota[None, :, None] < CAPACITY) & (expert_iota[None, None, :] == hot_expert[:, None, None]), 8 * EXPERTS, 0)
    scores = (noise_int + bias_int[None, None, :] + hot_bonus) * EXPERTS + expert_iota[None, None, :]
    expert_ids = lax.top_k(scores, TOP_K)[1].astype(jnp.int32)

    def rank_one(ids_dev):
        flat_ids = ids_dev.reshape(-1)
        onehot = (flat_ids[:, None] == expert_iota[None, :]).astype(jnp.int32)
        before = jnp.cumsum(onehot, axis=0) - onehot
        rank_pos = jnp.sum(before * onehot, axis=1)
        return rank_pos.reshape(TOKENS_DEV, TOP_K), jnp.sum(onehot, axis=0)

    rank_pos, n_total = lax.map(rank_one, expert_ids)
    slot_dev = jnp.where(rank_pos < CAPACITY, rank_pos, -1).astype(jnp.int32)
    pair_counts = jnp.minimum(n_total, CAPACITY).astype(jnp.int32)
    is_kept = slot_dev >= 0
    slot_safe = jnp.where(is_kept, slot_dev, CAPACITY)
    slot_clip = jnp.where(is_kept, slot_dev, 0)
    src_dev = jnp.broadcast_to(jnp.arange(GROUP_DEV, dtype=jnp.int32)[:, None, None], expert_ids.shape)

    w_gate = (jax.random.normal(weight_keys[0], (EXPERTS, MODEL_DIM, FFN_DIM), jnp.float32) * MODEL_DIM ** -0.5).astype(jnp.bfloat16)
    w_up = (jax.random.normal(weight_keys[1], (EXPERTS, MODEL_DIM, FFN_DIM), jnp.float32) * MODEL_DIM ** -0.5).astype(jnp.bfloat16)
    w_down = (jax.random.normal(weight_keys[2], (EXPERTS, FFN_DIM, MODEL_DIM), jnp.float32) * FFN_DIM ** -0.5).astype(jnp.bfloat16)
    x_tok = jax.random.normal(key_list[1], (GROUP_DEV, TOKENS_DEV, MODEL_DIM), jnp.float32).astype(jnp.bfloat16)
    stale_rows = jax.random.normal(key_list[2], (EXPERTS, GROUP_DEV, CAPACITY, MODEL_DIM), jnp.float32).astype(jnp.bfloat16)
    x_vals = jnp.broadcast_to(x_tok[:, :, None, :], (GROUP_DEV, TOKENS_DEV, TOP_K, MODEL_DIM))
    x_disp = stale_rows.at[expert_ids, src_dev, slot_safe].set(x_vals, mode="drop").reshape(EXPERTS, EXPERT_ROWS, MODEL_DIM)

    def forward_one(operands):
        x_rows, w_gate_e, w_up_e, w_down_e = operands
        h_g = jnp.dot(x_rows, w_gate_e, preferred_element_type=jnp.float32).astype(jnp.bfloat16)
        h_u = jnp.dot(x_rows, w_up_e, preferred_element_type=jnp.float32).astype(jnp.bfloat16)
        gate_f = h_g.astype(jnp.float32)
        hidden_act = (gate_f * jax.nn.sigmoid(gate_f) * h_u.astype(jnp.float32)).astype(jnp.bfloat16)
        y_rows = jnp.dot(hidden_act, w_down_e, preferred_element_type=jnp.float32).astype(jnp.bfloat16)
        return h_g, h_u, y_rows

    h_gate, h_up, y_exp = lax.map(forward_one, (x_disp, w_gate, w_up, w_down))
    y_pick = y_exp.reshape(EXPERTS, GROUP_DEV, CAPACITY, MODEL_DIM)[expert_ids, src_dev, slot_clip]
    y_routed = jnp.where(is_kept[..., None], y_pick, jnp.zeros((), jnp.bfloat16)).reshape(N_TOKENS, TOP_K, MODEL_DIM)
    grad_y = jax.random.normal(key_list[3], (N_TOKENS, MODEL_DIM), jnp.float32).astype(jnp.bfloat16)
    gate_vals = jax.random.uniform(key_list[4], (N_TOKENS, TOP_K), jnp.float32, 0.25, 1.0)
    return {"grad_y": grad_y, "gate_vals": gate_vals, "topk_idx": expert_ids.reshape(N_TOKENS, TOP_K), "slot_ids": slot_dev.reshape(N_TOKENS, TOP_K), "pair_counts": pair_counts, "y_routed": y_routed, "x_disp": x_disp, "h_gate": h_gate, "h_up": h_up, "w_gate": w_gate, "w_up": w_up, "w_down": w_down}


def reference(grad_y, gate_vals, topk_idx, slot_ids, pair_counts, y_routed, x_disp, h_gate, h_up, w_gate, w_up, w_down):
    grad_gate = jnp.einsum("td,tkd->tk", grad_y.astype(jnp.float32), y_routed.astype(jnp.float32))
    is_kept = slot_ids >= 0
    src_dev = jnp.broadcast_to((jnp.arange(N_TOKENS, dtype=jnp.int32) // TOKENS_DEV)[:, None], topk_idx.shape)
    slot_safe = jnp.where(is_kept, slot_ids, CAPACITY)
    slot_clip = jnp.where(is_kept, slot_ids, 0)
    gated_rows = (gate_vals[:, :, None] * grad_y.astype(jnp.float32)[:, None, :]).astype(jnp.bfloat16)
    disp_rows = jnp.zeros((EXPERTS, GROUP_DEV, CAPACITY, MODEL_DIM), jnp.bfloat16).at[topk_idx, src_dev, slot_safe].set(gated_rows, mode="drop")
    keep_row = jnp.arange(CAPACITY)[None, None, :] < jnp.transpose(pair_counts)[:, :, None]
    disp_rows = jnp.where(keep_row[..., None], disp_rows, jnp.zeros((), jnp.bfloat16)).reshape(EXPERTS, EXPERT_ROWS, MODEL_DIM)

    def expert_one(operands):
        grad_rows, x_rows, hg_rows, hu_rows, w_gate_e, w_up_e, w_down_e = operands
        grad_hidden = jnp.dot(grad_rows, w_down_e.T, preferred_element_type=jnp.float32).astype(jnp.bfloat16)
        gate_f = hg_rows.astype(jnp.float32)
        up_f = hu_rows.astype(jnp.float32)
        gate_sig = jax.nn.sigmoid(gate_f)
        gate_act = gate_f * gate_sig
        hidden_act = (gate_act * up_f).astype(jnp.bfloat16)
        grad_h = grad_hidden.astype(jnp.float32)
        grad_hgate = (grad_h * up_f * gate_sig * (1.0 + gate_f * (1.0 - gate_sig))).astype(jnp.bfloat16)
        grad_hup = (grad_h * gate_act).astype(jnp.bfloat16)
        grad_wdown = jnp.dot(hidden_act.T, grad_rows, preferred_element_type=jnp.float32)
        grad_wgate = jnp.dot(x_rows.T, grad_hgate, preferred_element_type=jnp.float32)
        grad_wup = jnp.dot(x_rows.T, grad_hup, preferred_element_type=jnp.float32)
        grad_disp = (jnp.dot(grad_hgate, w_gate_e.T, preferred_element_type=jnp.float32) + jnp.dot(grad_hup, w_up_e.T, preferred_element_type=jnp.float32)).astype(jnp.bfloat16)
        return grad_disp, grad_wgate, grad_wup, grad_wdown

    grad_disp, grad_w_gate, grad_w_up, grad_w_down = lax.map(expert_one, (disp_rows, x_disp, h_gate, h_up, w_gate, w_up, w_down))
    back_rows = grad_disp.reshape(EXPERTS, GROUP_DEV, CAPACITY, MODEL_DIM)[topk_idx, src_dev, slot_clip]
    grad_x = jnp.sum(jnp.where(is_kept[..., None], back_rows.astype(jnp.float32), 0.0), axis=1).astype(jnp.bfloat16)
    return grad_x, grad_gate, grad_w_gate, grad_w_up, grad_w_down
```

```python
import functools

import jax
import jax.numpy as jnp
from jax import lax
from jax.experimental import pallas as pl
from jax.experimental.pallas import tpu as pltpu
from jax.sharding import PartitionSpec as P

MESH = pl.DeviceIdType.MESH
F32 = jnp.float32
BF16 = jnp.bfloat16


def gather_kernel(n_dev, *refs):
    n_arr = 5
    ins, outs = refs[:n_arr], refs[n_arr:2 * n_arr]
    local_sem, send_sem, recv_sem = refs[2 * n_arr:]
    me = lax.axis_index("ep")
    local = [pltpu.make_async_copy(ins[i], outs[i].at[0], local_sem.at[i]) for i in range(n_arr)]
    for cp in local:
        cp.start()
    barrier = pltpu.get_barrier_semaphore()
    for k in range(1, n_dev):
        pl.semaphore_signal(barrier, inc=1, device_id={"ep": me ^ k}, device_id_type=MESH)
    pl.semaphore_wait(barrier, n_dev - 1)
    for cp in local:
        cp.wait()

    def remote(i, k, src_slot, dst_slot):
        return pltpu.make_async_remote_copy(
            src_ref=outs[i].at[src_slot], dst_ref=outs[i].at[dst_slot],
            send_sem=send_sem.at[i, dst_slot], recv_sem=recv_sem.at[i, dst_slot],
            device_id={"ep": me ^ k}, device_id_type=MESH)

    far = remote(0, 2, 0, 2)
    near = remote(0, 1, 0, 1)
    relay = remote(0, 1, 2, 3)
    small = [remote(i, k, 0, k) for k in (2, 3, 1) for i in range(1, n_arr)]
    far.start()
    near.start()
    for cp in small:
        cp.start()
    far.wait_recv()
    relay.start()
    near.wait()
    for cp in small:
        cp.wait()
    far.wait_send()
    relay.wait()


def gather_homes(arrays, n_dev):
    outs = [jax.ShapeDtypeStruct((n_dev,) + a.shape, a.dtype) for a in arrays]
    return pl.pallas_call(
        functools.partial(gather_kernel, n_dev),
        out_shape=outs,
        in_specs=[pl.BlockSpec(memory_space=pl.ANY)] * len(arrays),
        out_specs=[pl.BlockSpec(memory_space=pltpu.VMEM)] * len(arrays),
        scratch_shapes=[
            pltpu.SemaphoreType.DMA((len(arrays),)),
            pltpu.SemaphoreType.DMA((len(arrays), n_dev)),
            pltpu.SemaphoreType.DMA((len(arrays), n_dev)),
        ],
        compiler_params=pltpu.CompilerParams(collective_id=0, has_side_effects=True),
        name="gather_homes",
    )(*arrays)


def dot(a, b, ca, cb):
    return lax.dot_general(a, b, (((ca,), (cb,)), ((), ())), preferred_element_type=F32)


def expert_kernel(n_dev, cap, cnt_ref, gy_ref, tk_ref, sl_ref, gt_ref, hg_ref, hu_ref, wg_ref, wu_ref, wd_ref,
                  dwd_ref, dh1_ref, dh3_ref, *rest):
    part_refs = rest[:n_dev]
    key_ref, gate_ref, part_acc = rest[n_dev:]
    e = pl.program_id(0)
    n_loc = pl.num_programs(0)
    me = lax.axis_index("ep")
    expert = me * n_loc + e
    tok = sl_ref.shape[2]
    rows = n_dev * cap
    cols = n_dev * tok

    @pl.when(e == 0)
    def _():
        keys = [jnp.where(sl_ref[k] >= 0, tk_ref[k] * cap + sl_ref[k], -1) for k in range(n_dev)]
        key_ref[...] = jnp.concatenate(keys, axis=1)
        gate_ref[...] = jnp.concatenate([gt_ref[k] for k in range(n_dev)], axis=1)
        part_acc[...] = jnp.zeros_like(part_acc)

    row_id = lax.broadcasted_iota(jnp.int32, (rows, cols), 0)
    col_id = lax.broadcasted_iota(jnp.int32, (rows, cols), 1)
    target = jnp.where(((row_id // cap) ^ me) == col_id // tok, expert * cap + row_id % cap, -2)
    gate_sel = jnp.zeros((rows, cols), F32)
    pick = jnp.zeros((rows, cols), F32)
    for j in range(key_ref.shape[0]):
        hit = key_ref[j:j + 1, :] == target
        gate_sel = jnp.where(hit, gate_ref[j:j + 1, :], gate_sel)
        pick = jnp.where(hit, 1.0, pick)
    pick = pick.astype(BF16)
    row_gate = jnp.sum(gate_sel, axis=1, keepdims=True)
    row1 = lax.broadcasted_iota(jnp.int32, (rows, 1), 0)
    count = jnp.zeros((rows, 1), jnp.int32)
    for s in range(n_dev):
        count = jnp.where(row1 // cap == s, cnt_ref[s ^ me, expert], count)
    keep = row1 % cap < count
    gy_all = gy_ref[...].reshape(cols, gy_ref.shape[2])
    gated = dot(pick, gy_all, 1, 0) * row_gate
    grad_rows = jnp.where(keep, gated, 0.0).astype(BF16)

    gate_f = hg_ref[0].astype(F32)
    up_f = hu_ref[0].astype(F32)
    gate_sig = jax.nn.sigmoid(gate_f)
    gate_act = gate_f * gate_sig
    hidden_act = (gate_act * up_f).astype(BF16)
    grad_h = dot(grad_rows, wd_ref[0], 1, 1).astype(BF16).astype(F32)
    grad_hgate = (grad_h * up_f * gate_sig * (1.0 + gate_f * (1.0 - gate_sig))).astype(BF16)
    grad_hup = (grad_h * gate_act).astype(BF16)
    dh1_ref[0] = grad_hgate
    dh3_ref[0] = grad_hup
    dwd_ref[0] = dot(hidden_act, grad_rows, 0, 0)
    ret = (dot(grad_hgate, wg_ref[0], 1, 1) + dot(grad_hup, wu_ref[0], 1, 1)).astype(BF16)
    part_acc[...] += dot(pick, ret, 0, 0)

    @pl.when(e == n_loc - 1)
    def _():
        for k in range(n_dev):
            part_refs[k][...] = part_acc[k * tok:(k + 1) * tok, :]


def expert_pass(counts, gy, tk, sl, gt, hg, hu, wg, wu, wd, n_dev, cap):
    n_loc, ffn, model = wd.shape
    rows = hg.shape[1]
    tok = gy.shape[1]
    top_k = tk.shape[1]
    whole = lambda a: pl.BlockSpec(a.shape, lambda e: (0,) * a.ndim)
    per_e = lambda a: pl.BlockSpec((1,) + a.shape[1:], lambda e: (e, 0, 0))
    out_shape = [
        jax.ShapeDtypeStruct((n_loc, ffn, model), F32),
        jax.ShapeDtypeStruct((n_loc, rows, ffn), BF16),
        jax.ShapeDtypeStruct((n_loc, rows, ffn), BF16),
    ] + [jax.ShapeDtypeStruct((tok, model), F32)] * n_dev
    return pl.pallas_call(
        functools.partial(expert_kernel, n_dev, cap),
        grid=(n_loc,),
        out_shape=out_shape,
        in_specs=[pl.BlockSpec(memory_space=pltpu.SMEM), whole(gy), whole(tk), whole(sl), whole(gt),
                  per_e(hg), per_e(hu), per_e(wg), per_e(wu), per_e(wd)],
        out_specs=[per_e(out_shape[0]), per_e(out_shape[1]), per_e(out_shape[2])]
        + [pl.BlockSpec((tok, model), lambda e: (0, 0))] * n_dev,
        scratch_shapes=[
            pltpu.VMEM((top_k, n_dev * tok), jnp.int32),
            pltpu.VMEM((top_k, n_dev * tok), F32),
            pltpu.VMEM((n_dev * tok, model), F32),
        ],
        compiler_params=pltpu.CompilerParams(dimension_semantics=("arbitrary",), vmem_limit_bytes=48 * 2**20),
        cost_estimate=pl.CostEstimate(flops=10 * n_loc * rows * ffn * model, bytes_accessed=50 * 2**20, transcendentals=0),
        name="expert_pass",
    )(counts, gy, tk, sl, gt, hg, hu, wg, wu, wd)


def weight_kernel(x_ref, dh1_ref, dh3_ref, gy_ref, y_ref, dwg_ref, dwu_ref, gg_ref, gg_acc):
    e = pl.program_id(0)
    x = x_ref[0]
    dwg_ref[0] = dot(x, dh1_ref[0], 0, 0)
    dwu_ref[0] = dot(x, dh3_ref[0], 0, 0)
    prod = y_ref[...].astype(F32) * gy_ref[...].astype(F32)[:, None, :]
    step = y_ref.shape[0]
    gg_acc[pl.ds(pl.multiple_of(e * step, step), step), 0:y_ref.shape[1]] = jnp.sum(prod, axis=2)

    @pl.when(e == pl.num_programs(0) - 1)
    def _():
        gg_ref[...] = gg_acc[...].T[0:y_ref.shape[1], :]


def weight_pass(x, dh1, dh3, gy, y):
    n_loc, rows, model = x.shape
    ffn = dh1.shape[2]
    tok, top_k, _ = y.shape
    step = tok // n_loc
    per_e = lambda shape: pl.BlockSpec((1,) + shape[1:], lambda e: (e, 0, 0))
    grad_shape = jax.ShapeDtypeStruct((n_loc, model, ffn), F32)
    return pl.pallas_call(
        weight_kernel,
        grid=(n_loc,),
        out_shape=[grad_shape, grad_shape, jax.ShapeDtypeStruct((top_k, tok), F32)],
        in_specs=[per_e(x.shape), per_e(dh1.shape), per_e(dh3.shape),
                  pl.BlockSpec((step, model), lambda e: (e, 0)),
                  pl.BlockSpec((step, top_k, model), lambda e: (e, 0, 0))],
        out_specs=[per_e(grad_shape.shape), per_e(grad_shape.shape), pl.BlockSpec((top_k, tok), lambda e: (0, 0))],
        scratch_shapes=[pltpu.VMEM((tok, 128), F32)],
        compiler_params=pltpu.CompilerParams(dimension_semantics=("arbitrary",), vmem_limit_bytes=40 * 2**20),
        cost_estimate=pl.CostEstimate(flops=4 * n_loc * rows * ffn * model, bytes_accessed=40 * 2**20, transcendentals=0),
        name="weight_pass",
    )(x, dh1, dh3, gy, y)


def solution(mesh):
    n_dev = mesh.shape["ep"]
    rows_spec = P(("dp", "ep"), None)
    cube_spec = P(("dp", "ep"), None, None)
    weight_spec = P("ep", None, None)

    def local_step(grad_y, gate_vals, topk_idx, slot_ids, pair_counts, y_routed, x_disp, h_gate, h_up, w_gate, w_up, w_down):
        cap = x_disp.shape[1] // n_dev
        gy, tk, sl, gt, ct = gather_homes([grad_y, topk_idx.T, slot_ids.T, gate_vals.T, pair_counts], n_dev)
        dwd, dh1, dh3, *parts = expert_pass(ct[:, 0, :], gy, tk, sl, gt, h_gate, h_up, w_gate, w_up, w_down, n_dev, cap)
        back = [lax.ppermute(parts[k], "ep", [(i, i ^ k) for i in range(n_dev)]) for k in range(1, n_dev)]
        dwg, dwu, gg = weight_pass(x_disp, dh1, dh3, grad_y, y_routed)
        total = parts[0]
        for b in back:
            total = total + b
        return total.astype(BF16), gg.T, dwg, dwu, dwd

    return jax.shard_map(local_step, mesh=mesh, in_specs=(rows_spec, rows_spec, rows_spec, rows_spec, rows_spec, cube_spec, cube_spec, cube_spec, cube_spec, weight_spec, weight_spec, weight_spec), out_specs=(rows_spec, rows_spec, cube_spec, cube_spec, cube_spec), check_vma=False)
```

```python
import functools

import jax
import jax.numpy as jnp
from jax import lax
from jax.experimental import pallas as pl
from jax.experimental.pallas import tpu as pltpu
from jax.sharding import PartitionSpec as P

MESH = pl.DeviceIdType.MESH
F32 = jnp.float32
BF16 = jnp.bfloat16
ANY = pl.BlockSpec(memory_space=pl.ANY)
VMEM = pl.BlockSpec(memory_space=pltpu.VMEM)
MIB = 2**20


def dot(a, b, ca, cb):
    return lax.dot_general(a, b, (((ca,), (cb,)), ((), ())), preferred_element_type=F32)


def front_kernel(n_dev, n_tab, n_load, *refs):
    n_in = n_tab + n_load
    ins, outs = refs[:n_in], refs[n_in:2 * n_in]
    local_sem, send_sem, recv_sem = refs[2 * n_in:]
    me = lax.axis_index("ep")
    local = [pltpu.make_async_copy(ins[i], outs[i].at[0], local_sem.at[i]) for i in range(n_tab)]
    loads = [pltpu.make_async_copy(ins[i], outs[i], local_sem.at[i]) for i in range(n_tab, n_in)]
    for cp in local:
        cp.start()
    barrier = pltpu.get_barrier_semaphore()
    for k in range(1, n_dev):
        pl.semaphore_signal(barrier, inc=1, device_id={"ep": me ^ k}, device_id_type=MESH)
    for cp in loads:
        cp.start()
    pl.semaphore_wait(barrier, n_dev - 1)
    for cp in local:
        cp.wait()

    def remote(i, k, src_slot, dst_slot):
        return pltpu.make_async_remote_copy(
            src_ref=outs[i].at[src_slot], dst_ref=outs[i].at[dst_slot],
            send_sem=send_sem.at[i, dst_slot], recv_sem=recv_sem.at[i, dst_slot],
            device_id={"ep": me ^ k}, device_id_type=MESH)

    far = remote(0, 2, 0, 2)
    near = remote(0, 1, 0, 1)
    relay = remote(0, 1, 2, 3)
    small = [remote(i, k, 0, k) for k in (2, 3, 1) for i in range(1, n_tab)]
    far.start()
    near.start()
    for cp in small:
        cp.start()
    far.wait_recv()
    relay.start()
    near.wait()
    for cp in small:
        cp.wait()
    far.wait_send()
    relay.wait()
    for cp in loads:
        cp.wait()


def front_pass(tables, loads, n_dev):
    outs = [pltpu.VMEM((n_dev,) + a.shape, a.dtype) for a in tables] + [pltpu.VMEM(a.shape, a.dtype) for a in loads]
    n_in = len(outs)
    return pl.pallas_call(
        functools.partial(front_kernel, n_dev, len(tables), len(loads)),
        out_shape=outs,
        in_specs=[ANY] * n_in,
        out_specs=[VMEM] * n_in,
        scratch_shapes=[
            pltpu.SemaphoreType.DMA((n_in,)),
            pltpu.SemaphoreType.DMA((len(tables), n_dev)),
            pltpu.SemaphoreType.DMA((len(tables), n_dev)),
        ],
        compiler_params=pltpu.CompilerParams(collective_id=0, has_side_effects=True, vmem_limit_bytes=4 * MIB),
        name="front_pass",
    )(*[pltpu.with_memory_space_constraint(a, pltpu.HBM) for a in (*tables, *loads)])


def expert_kernel(n_dev, cap, gy_ref, tk_ref, sl_ref, gt_ref, ct_ref, hg_ref, hu_ref, wg_ref, wu_ref, wd_ref,
                  dwd_ref, dh1_ref, dh3_ref, *rest):
    part_refs = rest[:n_dev]
    key_ref, gate_ref = rest[n_dev:n_dev + 2]
    slots = [rest[n_dev + 2 + 6 * s:n_dev + 8 + 6 * s] for s in range(2)]
    out_sem = rest[n_dev + 14]
    n_loc = wd_ref.shape[0]
    me = lax.axis_index("ep")
    tok = sl_ref.shape[2]
    rows = n_dev * cap
    cols = n_dev * tok

    keys = [jnp.where(sl_ref[k] >= 0, tk_ref[k] * cap + sl_ref[k], -1) for k in range(n_dev)]
    key_ref[...] = jnp.concatenate(keys, axis=1)
    gate_ref[...] = jnp.concatenate([gt_ref[k] for k in range(n_dev)], axis=1)
    for k in range(n_dev):
        part_refs[k][...] = jnp.zeros_like(part_refs[k])

    def out_copy(e, s):
        return pltpu.make_async_copy(slots[s][5], dwd_ref.at[e], out_sem.at[s])

    def front(e, s):
        pick_s, act_s, grad_s, dh1_s, dh3_s, _ = slots[s]
        expert = me * n_loc + e
        row_id = lax.broadcasted_iota(jnp.int32, (rows, cols), 0)
        col_id = lax.broadcasted_iota(jnp.int32, (rows, cols), 1)
        target = jnp.where(((row_id // cap) ^ me) == col_id // tok, expert * cap + row_id % cap, -2)
        gate_sel = jnp.zeros((rows, cols), F32)
        pick = jnp.zeros((rows, cols), F32)
        for j in range(key_ref.shape[0]):
            hit = key_ref[j:j + 1, :] == target
            gate_sel = jnp.where(hit, gate_ref[j:j + 1, :], gate_sel)
            pick = jnp.where(hit, 1.0, pick)
        pick = pick.astype(BF16)
        row_gate = jnp.sum(gate_sel, axis=1, keepdims=True)
        row1 = lax.broadcasted_iota(jnp.int32, (rows, 1), 0)
        lane = lax.broadcasted_iota(jnp.int32, ct_ref.shape[1:], 1)
        count = jnp.zeros((rows, 1), jnp.int32)
        for k in range(n_dev):
            here = jnp.sum(jnp.where(lane == expert, ct_ref[k], 0), axis=1, keepdims=True)
            count = jnp.where((row1 // cap) ^ me == k, here, count)
        gated = dot(pick, gy_ref[...].reshape(cols, gy_ref.shape[2]), 1, 0) * row_gate
        grad_rows = jnp.where(row1 % cap < count, gated, 0.0).astype(BF16)
        gate_f = hg_ref[e].astype(F32)
        up_f = hu_ref[e].astype(F32)
        gate_sig = jax.nn.sigmoid(gate_f)
        gate_act = gate_f * gate_sig
        grad_h = dot(grad_rows, wd_ref[e], 1, 1).astype(BF16).astype(F32)
        grad_hgate = (grad_h * up_f * gate_sig * (1.0 + gate_f * (1.0 - gate_sig))).astype(BF16)
        grad_hup = (grad_h * gate_act).astype(BF16)
        pick_s[...] = pick
        act_s[...] = (gate_act * up_f).astype(BF16)
        grad_s[...] = grad_rows
        dh1_s[...] = grad_hgate
        dh3_s[...] = grad_hup
        dh1_ref[e] = grad_hgate
        dh3_ref[e] = grad_hup

    def back(e, s):
        pick_s, act_s, grad_s, dh1_s, dh3_s, stage = slots[s]
        ret = (dot(dh1_s[...], wg_ref[e], 1, 1) + dot(dh3_s[...], wu_ref[e], 1, 1)).astype(BF16)
        part = dot(pick_s[...], ret, 0, 0)
        for k in range(n_dev):
            part_refs[k][...] += part[k * tok:(k + 1) * tok, :]
        stage[...] = dot(act_s[...], grad_s[...], 0, 0)
        out_copy(e, s).start()

    def pair(i, last):
        e = 2 * i

        @pl.when(i > 0)
        def _():
            out_copy(e, 0).wait()

        front(e + 1, 1)
        back(e, 0)

        @pl.when(i > 0)
        def _():
            out_copy(e, 1).wait()

        if not last:
            front(e + 2, 0)
        back(e + 1, 1)

    front(0, 0)

    def body(i, carry):
        pair(i, False)
        return carry

    lax.fori_loop(0, n_loc // 2 - 1, body, 0)
    pair(n_loc // 2 - 1, True)
    out_copy(0, 0).wait()
    out_copy(0, 1).wait()


def expert_pass(gy, tk, sl, gt, ct, hg, hu, wg, wu, wd, n_dev, cap):
    n_loc, ffn, model = wd.shape
    rows = hg.shape[1]
    tok = gy.shape[1]
    top_k = tk.shape[1]
    slot = [
        pltpu.VMEM((rows, n_dev * tok), BF16),
        pltpu.VMEM((rows, ffn), BF16),
        pltpu.VMEM((rows, model), BF16),
        pltpu.VMEM((rows, ffn), BF16),
        pltpu.VMEM((rows, ffn), BF16),
        pltpu.VMEM((ffn, model), F32),
    ]
    return pl.pallas_call(
        functools.partial(expert_kernel, n_dev, cap),
        out_shape=[
            jax.ShapeDtypeStruct((n_loc, ffn, model), F32),
            pltpu.VMEM((n_loc, rows, ffn), BF16),
            pltpu.VMEM((n_loc, rows, ffn), BF16),
        ] + [pltpu.VMEM((tok, model), F32)] * n_dev,
        in_specs=[VMEM] * 10,
        out_specs=[ANY, VMEM, VMEM] + [VMEM] * n_dev,
        scratch_shapes=[
            pltpu.VMEM((top_k, n_dev * tok), jnp.int32),
            pltpu.VMEM((top_k, n_dev * tok), F32),
        ] + slot + slot + [pltpu.SemaphoreType.DMA((2,))],
        compiler_params=pltpu.CompilerParams(vmem_limit_bytes=EXPERT_VMEM),
        cost_estimate=pl.CostEstimate(flops=10 * n_loc * rows * ffn * model, bytes_accessed=50 * MIB, transcendentals=0),
        name="expert_pass",
    )(gy, tk, sl, gt, ct, hg, hu, wg, wu, wd)


EXPERT_VMEM = 14 * MIB
WEIGHT_VMEM = 20 * MIB


def weight_kernel(x_ref, dh1_ref, dh3_ref, gy_ref, y_ref, dwg_ref, dwu_ref, gg_ref, stage, gg_acc, out_sem, gg_sem):
    n_loc, _, model = x_ref.shape
    top_k = y_ref.shape[1]
    half = model // 2

    def out_copy(e, s, q):
        dst = (dwg_ref, dwu_ref)[q % 2].at[e, pl.ds(half * (q // 2), half), :]
        return pltpu.make_async_copy(stage.at[s, q], dst, out_sem.at[s, q])

    def one(e, s):
        for h in range(2):
            x = x_ref[e, :, h * half:(h + 1) * half]
            for w, dh in enumerate((dh1_ref, dh3_ref)):
                q = 2 * h + w
                stage[s, q] = dot(x, dh[e], 0, 0)
                out_copy(e, s, q).start()

    def wait_all(s):
        for q in range(4):
            out_copy(0, s, q).wait()

    def body(i, carry):
        for s in range(2):
            @pl.when(i > 0)
            def _():
                wait_all(s)
            one(2 * i + s, s)

        @pl.when(i == n_loc // 2 - 2)
        def _():
            step = 8
            for b in range(y_ref.shape[0] // step):
                prod = y_ref[b * step:(b + 1) * step].astype(F32) * gy_ref[0, b * step:(b + 1) * step].astype(F32)[:, None, :]
                gg_acc[b * step:(b + 1) * step, 0:top_k] = jnp.sum(prod, axis=2)
            gg_ref[...] = gg_acc[...].T[0:top_k, :]
        return carry

    lax.fori_loop(0, n_loc // 2, body, 0)
    wait_all(0)
    wait_all(1)


def weight_pass(x, dh1, dh3, gy, y):
    n_loc, rows, model = x.shape
    ffn = dh1.shape[2]
    tok, top_k, _ = y.shape
    grad_shape = jax.ShapeDtypeStruct((n_loc, model, ffn), F32)
    return pl.pallas_call(
        weight_kernel,
        out_shape=[grad_shape, grad_shape, jax.ShapeDtypeStruct((top_k, tok), F32)],
        in_specs=[VMEM] * 5,
        out_specs=[ANY, ANY, VMEM],
        scratch_shapes=[
            pltpu.VMEM((2, 4, model // 2, ffn), F32),
            pltpu.VMEM((tok, 128), F32),
            pltpu.SemaphoreType.DMA((2, 4)),
            pltpu.SemaphoreType.DMA,
        ],
        compiler_params=pltpu.CompilerParams(vmem_limit_bytes=WEIGHT_VMEM),
        cost_estimate=pl.CostEstimate(flops=4 * n_loc * rows * ffn * model, bytes_accessed=40 * MIB, transcendentals=0),
        name="weight_pass",
    )(x, dh1, dh3, gy, y)


def solution(mesh):
    n_dev = mesh.shape["ep"]
    rows_spec = P(("dp", "ep"), None)
    cube_spec = P(("dp", "ep"), None, None)
    weight_spec = P("ep", None, None)

    def local_step(grad_y, gate_vals, topk_idx, slot_ids, pair_counts, y_routed, x_disp, h_gate, h_up, w_gate, w_up, w_down):
        cap = x_disp.shape[1] // n_dev
        tables = [grad_y, topk_idx.T, slot_ids.T, gate_vals.T, pair_counts]
        loads = [w_down, h_gate, h_up, w_gate, w_up, x_disp, y_routed]
        gy, tk, sl, gt, ct, wd, hg, hu, wg, wu, x, y = front_pass(tables, loads, n_dev)
        dwd, dh1, dh3, *parts = expert_pass(gy, tk, sl, gt, ct, hg, hu, wg, wu, wd, n_dev, cap)
        back = [lax.ppermute(parts[k], "ep", [(i, i ^ k) for i in range(n_dev)]) for k in range(1, n_dev)]
        dwg, dwu, gg = weight_pass(x, dh1, dh3, gy, y)
        total = parts[0]
        for b in back:
            total = total + b
        return total.astype(BF16), gg.T, dwg, dwu, dwd

    return jax.shard_map(local_step, mesh=mesh, in_specs=(rows_spec, rows_spec, rows_spec, rows_spec, rows_spec, cube_spec, cube_spec, cube_spec, cube_spec, weight_spec, weight_spec, weight_spec), out_specs=(rows_spec, rows_spec, cube_spec, cube_spec, cube_spec), check_vma=False)
```

```python
import functools

import jax
import jax.numpy as jnp
from jax import lax
from jax.experimental import pallas as pl
from jax.experimental.pallas import tpu as pltpu
from jax.sharding import PartitionSpec as P

MESH = pl.DeviceIdType.MESH
F32 = jnp.float32
BF16 = jnp.bfloat16
ANY = pl.BlockSpec(memory_space=pl.ANY)
VMEM = pl.BlockSpec(memory_space=pltpu.VMEM)
MIB = 2**20
SPLIT = 4


def dot(a, b, ca, cb):
    return lax.dot_general(a, b, (((ca,), (cb,)), ((), ())), preferred_element_type=F32)


def front_kernel(n_dev, cap, gy_in, tk_in, sl_in, gt_in, ct_in, hg_in, hu_in, wd_in, wg_in, wu_in, x_in, y_in,
                 gy_ref, pick_ref, d_ref, act_ref, fac1_ref, fac3_ref, wd_ref, wg_ref, wu_ref, x_ref, y_ref,
                 tk_ref, sl_ref, gt_ref, ct_ref, hg_ref, hu_ref, gate_ref, local_sem, load_sem, send_sem, recv_sem):
    me = lax.axis_index("ep")
    n_loc = d_ref.shape[0]
    bufs = [gy_ref, tk_ref, sl_ref, gt_ref, ct_ref]
    local = [pltpu.make_async_copy(a, b.at[0], local_sem.at[i])
             for i, (a, b) in enumerate(zip((gy_in, tk_in, sl_in, gt_in, ct_in), bufs))]
    pairs = [(hg_in, hg_ref), (hu_in, hu_ref), (wd_in, wd_ref), (wg_in.at[pl.ds(0, SPLIT)], wg_ref),
             (wu_in.at[pl.ds(0, SPLIT)], wu_ref), (x_in, x_ref), (y_in, y_ref)]
    loads = [pltpu.make_async_copy(a, b, load_sem.at[i]) for i, (a, b) in enumerate(pairs)]
    for cp in local:
        cp.start()
    barrier = pltpu.get_barrier_semaphore()
    for k in range(1, n_dev):
        pl.semaphore_signal(barrier, inc=1, device_id={"ep": me ^ k}, device_id_type=MESH)
    for cp in loads:
        cp.start()
    pl.semaphore_wait(barrier, n_dev - 1)
    for cp in local:
        cp.wait()

    def remote(i, k, src_slot, dst_slot):
        return pltpu.make_async_remote_copy(
            src_ref=bufs[i].at[src_slot], dst_ref=bufs[i].at[dst_slot],
            send_sem=send_sem.at[i, dst_slot], recv_sem=recv_sem.at[i, dst_slot],
            device_id={"ep": me ^ k}, device_id_type=MESH)

    far = remote(0, 2, 0, 2)
    near = remote(0, 1, 0, 1)
    relay = remote(0, 1, 2, 3)
    small = {k: [remote(i, k, 0, k) for i in range(1, len(bufs))] for k in range(1, n_dev)}
    for cp in small[2]:
        cp.start()
    far.start()
    for k in (3, 1):
        for cp in small[k]:
            cp.start()
    near.start()

    loads[0].wait()
    loads[1].wait()

    def silu(e, carry):
        gate_f = hg_ref[e].astype(F32)
        up_f = hu_ref[e].astype(F32)
        gate_sig = jax.nn.sigmoid(gate_f)
        gate_act = gate_f * gate_sig
        act_ref[e] = (gate_act * up_f).astype(BF16)
        fac1_ref[e] = up_f * gate_sig * (1.0 + gate_f * (1.0 - gate_sig))
        fac3_ref[e] = gate_act
        return carry

    lax.fori_loop(0, n_loc, silu, 0)

    tok = tk_ref.shape[2]
    rows = n_loc * cap

    def select(k):
        row = lax.broadcasted_iota(jnp.int32, (rows, tok), 0) + me * rows
        key = jnp.where(sl_ref[k] >= 0, tk_ref[k] * cap + sl_ref[k], -1)
        gate = gt_ref[k]
        pick = jnp.zeros((rows, tok), F32)
        gate_sel = jnp.zeros((rows, tok), F32)
        for j in range(key.shape[0]):
            hit = key[j:j + 1, :] == row
            pick = jnp.where(hit, 1.0, pick)
            gate_sel = jnp.where(hit, gate[j:j + 1, :], gate_sel)
        row1 = lax.broadcasted_iota(jnp.int32, (rows, 1), 0)
        lane = lax.broadcasted_iota(jnp.int32, ct_ref.shape[1:], 1)
        count = jnp.zeros((rows, 1), jnp.int32)
        for e in range(n_loc):
            here = jnp.sum(jnp.where(lane == me * n_loc + e, ct_ref[k], 0), axis=1, keepdims=True)
            count = jnp.where(row1 // cap == e, here, count)
        pick_ref[k] = pick.astype(BF16)
        gate_ref[k] = jnp.where(row1 % cap < count, jnp.sum(gate_sel, axis=1, keepdims=True), 0.0)

    def gated_rows(k):
        rows_k = (dot(pick_ref[k], gy_ref[k], 1, 0) * gate_ref[k]).astype(BF16)
        at = pl.multiple_of((me ^ k) * cap, cap)
        for e in range(n_loc):
            d_ref[e, pl.ds(at, cap), :] = rows_k[e * cap:(e + 1) * cap, :]

    select(0)
    gated_rows(0)
    for k in (1, 2, 3):
        for cp in small[k]:
            cp.wait()
        select(k)
    near.wait()
    gated_rows(1)
    far.wait_recv()
    relay.start()
    gated_rows(2)
    relay.wait()
    gated_rows(3)
    far.wait_send()
    for cp in loads[2:]:
        cp.wait()


def front_pass(gy, tk, sl, gt, ct, hg, hu, wd, wg, wu, x, y, n_dev, cap):
    args = (gy, tk, sl, gt, ct, hg, hu, wd, wg, wu, x, y)
    n_loc, ffn, model = wd.shape
    tok = gy.shape[0]
    rows = hg.shape[1]
    outs = [
        pltpu.VMEM((n_dev, tok, model), BF16),
        pltpu.VMEM((n_dev, n_loc * cap, tok), BF16),
        pltpu.VMEM((n_loc, rows, model), BF16),
        pltpu.VMEM((n_loc, rows, ffn), BF16),
        pltpu.VMEM((n_loc, rows, ffn), F32),
        pltpu.VMEM((n_loc, rows, ffn), F32),
        pltpu.VMEM(wd.shape, BF16),
        pltpu.VMEM((SPLIT,) + wg.shape[1:], BF16),
        pltpu.VMEM((SPLIT,) + wu.shape[1:], BF16),
        pltpu.VMEM(x.shape, BF16),
        pltpu.VMEM(y.shape, BF16),
    ]
    return pl.pallas_call(
        functools.partial(front_kernel, n_dev, cap),
        out_shape=outs,
        in_specs=[ANY] * len(args),
        out_specs=[VMEM] * len(outs),
        scratch_shapes=[
            pltpu.VMEM((n_dev,) + tk.shape, jnp.int32),
            pltpu.VMEM((n_dev,) + sl.shape, jnp.int32),
            pltpu.VMEM((n_dev,) + gt.shape, F32),
            pltpu.VMEM((n_dev,) + ct.shape, jnp.int32),
            pltpu.VMEM(hg.shape, BF16),
            pltpu.VMEM(hu.shape, BF16),
            pltpu.VMEM((n_dev, n_loc * cap, 1), F32),
            pltpu.SemaphoreType.DMA((5,)),
            pltpu.SemaphoreType.DMA((7,)),
            pltpu.SemaphoreType.DMA((5, n_dev)),
            pltpu.SemaphoreType.DMA((5, n_dev)),
        ],
        compiler_params=pltpu.CompilerParams(collective_id=0, has_side_effects=True, vmem_limit_bytes=8 * MIB),
        name="front_pass",
    )(*[pltpu.with_memory_space_constraint(a, pltpu.HBM) for a in args])


def expert_kernel(n_dev, cap, pick_ref, d_ref, act_ref, fac1_ref, fac3_ref, wd_ref, wga_ref, wua_ref, wg_in, wu_in,
                  dwd_ref, dh1_ref, dh3_ref, *rest):
    part_refs = rest[:n_dev]
    wgb_ref, wub_ref, ret_ref, stage_ref, load_sem, out_sem = rest[n_dev:]
    n_loc = wd_ref.shape[0]
    n_stage = stage_ref.shape[0]
    me = lax.axis_index("ep")
    loads = {e: (pltpu.make_async_copy(wg_in.at[e], wgb_ref.at[e - SPLIT], load_sem.at[0, e - SPLIT]),
                 pltpu.make_async_copy(wu_in.at[e], wub_ref.at[e - SPLIT], load_sem.at[1, e - SPLIT]))
             for e in range(SPLIT, n_loc)}
    for e in loads:
        for cp in loads[e]:
            cp.start()
    outs = [pltpu.make_async_copy(stage_ref.at[e % n_stage], dwd_ref.at[e], out_sem.at[e % n_stage]) for e in range(n_loc)]

    def down_grad(e):
        if e >= n_stage:
            outs[e - n_stage].wait()
        stage_ref[e % n_stage] = dot(act_ref[e], d_ref[e], 0, 0)
        outs[e].start()

    def hidden_grad(e):
        grad_h = dot(d_ref[e], wd_ref[e], 1, 1).astype(BF16).astype(F32)
        dh1_ref[e] = (grad_h * fac1_ref[e]).astype(BF16)
        dh3_ref[e] = (grad_h * fac3_ref[e]).astype(BF16)

    def row_grad(e):
        if e in loads:
            for cp in loads[e]:
                cp.wait()
        wg, wu = (wgb_ref[e - SPLIT], wub_ref[e - SPLIT]) if e in loads else (wga_ref[e], wua_ref[e])
        ret = (dot(dh1_ref[e], wg, 1, 1) + dot(dh3_ref[e], wu, 1, 1)).astype(BF16)
        for s in range(n_dev):
            ret_ref[s, e * cap:(e + 1) * cap, :] = ret[s * cap:(s + 1) * cap, :]

    down_grad(0)
    hidden_grad(0)
    for e in range(n_loc):
        if e + 1 < n_loc:
            down_grad(e + 1)
            hidden_grad(e + 1)
        row_grad(e)
    for k in range(n_dev):
        part_refs[k][...] = dot(pick_ref[k], ret_ref[me ^ k], 0, 0)
    for e in range(n_loc - n_stage, n_loc):
        outs[e].wait()


def expert_pass(pick, d, act, fac1, fac3, wd, wga, wua, wg, wu, n_dev, cap):
    n_loc, ffn, model = wd.shape
    rows = d.shape[1]
    tok = pick.shape[2]
    n_stage = 2
    late = n_loc - SPLIT
    hbm = [pltpu.with_memory_space_constraint(a, pltpu.HBM) for a in (wg, wu)]
    return pl.pallas_call(
        functools.partial(expert_kernel, n_dev, cap),
        out_shape=[
            jax.ShapeDtypeStruct((n_loc, ffn, model), F32),
            pltpu.VMEM((n_loc, rows, ffn), BF16),
            pltpu.VMEM((n_loc, rows, ffn), BF16),
        ] + [pltpu.VMEM((tok, model), F32)] * n_dev,
        in_specs=[VMEM] * 8 + [ANY] * 2,
        out_specs=[ANY, VMEM, VMEM] + [VMEM] * n_dev,
        scratch_shapes=[
            pltpu.VMEM((late,) + wg.shape[1:], BF16),
            pltpu.VMEM((late,) + wu.shape[1:], BF16),
            pltpu.VMEM((n_dev, n_loc * cap, model), BF16),
            pltpu.VMEM((n_stage, ffn, model), F32),
            pltpu.SemaphoreType.DMA((2, late)),
            pltpu.SemaphoreType.DMA((n_stage,)),
        ],
        compiler_params=pltpu.CompilerParams(vmem_limit_bytes=20 * MIB),
        cost_estimate=pl.CostEstimate(flops=10 * n_loc * rows * ffn * model, bytes_accessed=50 * MIB, transcendentals=0),
        name="expert_pass",
    )(pick, d, act, fac1, fac3, wd, wga, wua, *hbm)


def weight_kernel(x_ref, dh1_ref, dh3_ref, gy_ref, y_ref, dwg_ref, dwu_ref, gg_ref, stage, gg_acc, out_sem):
    n_loc, _, model = x_ref.shape
    top_k = y_ref.shape[1]
    half = model // 2

    def out_copy(e, s, q):
        dst = (dwg_ref, dwu_ref)[q % 2].at[e, pl.ds(half * (q // 2), half), :]
        return pltpu.make_async_copy(stage.at[s, q], dst, out_sem.at[s, q])

    def one(e, s):
        for h in range(2):
            x = x_ref[e, :, h * half:(h + 1) * half]
            for w, dh in enumerate((dh1_ref, dh3_ref)):
                q = 2 * h + w
                stage[s, q] = dot(x, dh[e], 0, 0)
                out_copy(e, s, q).start()

    def wait_all(s):
        for q in range(4):
            out_copy(0, s, q).wait()

    def body(i, carry):
        for s in range(2):
            @pl.when(i > 0)
            def _():
                wait_all(s)
            one(2 * i + s, s)

        @pl.when(i == n_loc // 2 - 2)
        def _():
            step = 8
            for b in range(y_ref.shape[0] // step):
                prod = y_ref[b * step:(b + 1) * step].astype(F32) * gy_ref[0, b * step:(b + 1) * step].astype(F32)[:, None, :]
                gg_acc[b * step:(b + 1) * step, 0:top_k] = jnp.sum(prod, axis=2)
            gg_ref[...] = gg_acc[...].T[0:top_k, :]
        return carry

    lax.fori_loop(0, n_loc // 2, body, 0)
    wait_all(0)
    wait_all(1)


def weight_pass(x, dh1, dh3, gy, y):
    n_loc, rows, model = x.shape
    ffn = dh1.shape[2]
    tok, top_k, _ = y.shape
    grad_shape = jax.ShapeDtypeStruct((n_loc, model, ffn), F32)
    return pl.pallas_call(
        weight_kernel,
        out_shape=[grad_shape, grad_shape, jax.ShapeDtypeStruct((top_k, tok), F32)],
        in_specs=[VMEM] * 5,
        out_specs=[ANY, ANY, VMEM],
        scratch_shapes=[
            pltpu.VMEM((2, 4, model // 2, ffn), F32),
            pltpu.VMEM((tok, 128), F32),
            pltpu.SemaphoreType.DMA((2, 4)),
        ],
        compiler_params=pltpu.CompilerParams(vmem_limit_bytes=20 * MIB),
        cost_estimate=pl.CostEstimate(flops=4 * n_loc * rows * ffn * model, bytes_accessed=40 * MIB, transcendentals=0),
        name="weight_pass",
    )(x, dh1, dh3, gy, y)


def solution(mesh):
    n_dev = mesh.shape["ep"]
    rows_spec = P(("dp", "ep"), None)
    cube_spec = P(("dp", "ep"), None, None)
    weight_spec = P("ep", None, None)

    def local_step(grad_y, gate_vals, topk_idx, slot_ids, pair_counts, y_routed, x_disp, h_gate, h_up, w_gate, w_up, w_down):
        cap = x_disp.shape[1] // n_dev
        gy, pick, d, act, fac1, fac3, wd, wga, wua, x, y = front_pass(
            grad_y, topk_idx.T, slot_ids.T, gate_vals.T, pair_counts, h_gate, h_up, w_down, w_gate, w_up, x_disp, y_routed, n_dev, cap)
        dwd, dh1, dh3, *parts = expert_pass(pick, d, act, fac1, fac3, wd, wga, wua, w_gate, w_up, n_dev, cap)
        back = [lax.ppermute(parts[k], "ep", [(i, i ^ k) for i in range(n_dev)]) for k in range(1, n_dev)]
        dwg, dwu, gg = weight_pass(x, dh1, dh3, gy, y)
        total = parts[0]
        for b in back:
            total = total + b
        return total.astype(BF16), gg.T, dwg, dwu, dwd

    return jax.shard_map(local_step, mesh=mesh, in_specs=(rows_spec, rows_spec, rows_spec, rows_spec, rows_spec, cube_spec, cube_spec, cube_spec, cube_spec, weight_spec, weight_spec, weight_spec), out_specs=(rows_spec, rows_spec, cube_spec, cube_spec, cube_spec), check_vma=False)
```

```python
import functools

import jax
import jax.numpy as jnp
from jax import lax
from jax.experimental import pallas as pl
from jax.experimental.pallas import tpu as pltpu
from jax.sharding import PartitionSpec as P

MESH = pl.DeviceIdType.MESH
F32 = jnp.float32
BF16 = jnp.bfloat16
ANY = pl.BlockSpec(memory_space=pl.ANY)
VMEM = pl.BlockSpec(memory_space=pltpu.VMEM)
MIB = 2**20
SPLIT = 5


def dot(a, b, ca, cb):
    return lax.dot_general(a, b, (((ca,), (cb,)), ((), ())), preferred_element_type=F32)


def front_kernel(n_dev, cap, gy_in, tk_in, sl_in, gt_in, ct_in, hg_in, hu_in, wd_in, wg_in, wu_in, x_in, y_in,
                 gy_ref, pick_ref, d_ref, act_ref, fac1_ref, fac3_ref, wd_ref, wg_ref, wu_ref, x_ref, y_ref,
                 tk_ref, sl_ref, gt_ref, ct_ref, hg_ref, hu_ref, gate_ref, local_sem, load_sem, send_sem, recv_sem):
    me = lax.axis_index("ep")
    n_loc = d_ref.shape[0]
    bufs = [gy_ref, tk_ref, sl_ref, gt_ref, ct_ref]
    local = [pltpu.make_async_copy(a, b.at[0], local_sem.at[i])
             for i, (a, b) in enumerate(zip((gy_in, tk_in, sl_in, gt_in, ct_in), bufs))]
    pairs = [(hg_in, hg_ref), (hu_in, hu_ref), (wd_in, wd_ref), (wg_in.at[pl.ds(0, SPLIT)], wg_ref),
             (wu_in.at[pl.ds(0, SPLIT)], wu_ref), (x_in, x_ref), (y_in, y_ref)]
    loads = [pltpu.make_async_copy(a, b, load_sem.at[i]) for i, (a, b) in enumerate(pairs)]
    for cp in local:
        cp.start()
    barrier = pltpu.get_barrier_semaphore()
    for k in range(1, n_dev):
        pl.semaphore_signal(barrier, inc=1, device_id={"ep": me ^ k}, device_id_type=MESH)
    for cp in loads:
        cp.start()
    pl.semaphore_wait(barrier, n_dev - 1)
    for cp in local:
        cp.wait()

    def remote(i, k, src_slot, dst_slot):
        return pltpu.make_async_remote_copy(
            src_ref=bufs[i].at[src_slot], dst_ref=bufs[i].at[dst_slot],
            send_sem=send_sem.at[i, dst_slot], recv_sem=recv_sem.at[i, dst_slot],
            device_id={"ep": me ^ k}, device_id_type=MESH)

    far = remote(0, 2, 0, 2)
    near = remote(0, 1, 0, 1)
    relay = remote(0, 1, 2, 3)
    small = {k: [remote(i, k, 0, k) for i in range(1, len(bufs))] for k in range(1, n_dev)}
    for cp in small[2]:
        cp.start()
    far.start()
    for k in (3, 1):
        for cp in small[k]:
            cp.start()
    near.start()

    loads[0].wait()
    loads[1].wait()

    def silu(e, carry):
        gate_f = hg_ref[e].astype(F32)
        up_f = hu_ref[e].astype(F32)
        gate_sig = jax.nn.sigmoid(gate_f)
        gate_act = gate_f * gate_sig
        act_ref[e] = (gate_act * up_f).astype(BF16)
        fac1_ref[e] = up_f * gate_sig * (1.0 + gate_f * (1.0 - gate_sig))
        fac3_ref[e] = gate_act
        return carry

    lax.fori_loop(0, n_loc, silu, 0)

    tok = tk_ref.shape[2]
    rows = n_loc * cap

    def select(k):
        row = lax.broadcasted_iota(jnp.int32, (rows, tok), 0) + me * rows
        key = jnp.where(sl_ref[k] >= 0, tk_ref[k] * cap + sl_ref[k], -1)
        gate = gt_ref[k]
        pick = jnp.zeros((rows, tok), F32)
        gate_sel = jnp.zeros((rows, tok), F32)
        for j in range(key.shape[0]):
            hit = key[j:j + 1, :] == row
            pick = jnp.where(hit, 1.0, pick)
            gate_sel = jnp.where(hit, gate[j:j + 1, :], gate_sel)
        row1 = lax.broadcasted_iota(jnp.int32, (rows, 1), 0)
        lane = lax.broadcasted_iota(jnp.int32, ct_ref.shape[1:], 1)
        count = jnp.zeros((rows, 1), jnp.int32)
        for e in range(n_loc):
            here = jnp.sum(jnp.where(lane == me * n_loc + e, ct_ref[k], 0), axis=1, keepdims=True)
            count = jnp.where(row1 // cap == e, here, count)
        pick_ref[k] = pick.astype(BF16)
        gate_ref[k] = jnp.where(row1 % cap < count, jnp.sum(gate_sel, axis=1, keepdims=True), 0.0)

    def gated_rows(k):
        rows_k = (dot(pick_ref[k], gy_ref[k], 1, 0) * gate_ref[k]).astype(BF16)
        at = pl.multiple_of((me ^ k) * cap, cap)
        for e in range(n_loc):
            d_ref[e, pl.ds(at, cap), :] = rows_k[e * cap:(e + 1) * cap, :]

    select(0)
    gated_rows(0)
    for k in (1, 2, 3):
        for cp in small[k]:
            cp.wait()
        select(k)
    near.wait()
    gated_rows(1)
    far.wait_recv()
    relay.start()
    gated_rows(2)
    relay.wait()
    gated_rows(3)
    far.wait_send()
    for cp in loads[2:]:
        cp.wait()


def front_pass(gy, tk, sl, gt, ct, hg, hu, wd, wg, wu, x, y, n_dev, cap):
    args = (gy, tk, sl, gt, ct, hg, hu, wd, wg, wu, x, y)
    n_loc, ffn, model = wd.shape
    tok = gy.shape[0]
    rows = hg.shape[1]
    outs = [
        pltpu.VMEM((n_dev, tok, model), BF16),
        pltpu.VMEM((n_dev, n_loc * cap, tok), BF16),
        pltpu.VMEM((n_loc, rows, model), BF16),
        pltpu.VMEM((n_loc, rows, ffn), BF16),
        pltpu.VMEM((n_loc, rows, ffn), F32),
        pltpu.VMEM((n_loc, rows, ffn), F32),
        pltpu.VMEM(wd.shape, BF16),
        pltpu.VMEM((SPLIT,) + wg.shape[1:], BF16),
        pltpu.VMEM((SPLIT,) + wu.shape[1:], BF16),
        pltpu.VMEM(x.shape, BF16),
        pltpu.VMEM(y.shape, BF16),
    ]
    return pl.pallas_call(
        functools.partial(front_kernel, n_dev, cap),
        out_shape=outs,
        in_specs=[ANY] * len(args),
        out_specs=[VMEM] * len(outs),
        scratch_shapes=[
            pltpu.VMEM((n_dev,) + tk.shape, jnp.int32),
            pltpu.VMEM((n_dev,) + sl.shape, jnp.int32),
            pltpu.VMEM((n_dev,) + gt.shape, F32),
            pltpu.VMEM((n_dev,) + ct.shape, jnp.int32),
            pltpu.VMEM(hg.shape, BF16),
            pltpu.VMEM(hu.shape, BF16),
            pltpu.VMEM((n_dev, n_loc * cap, 1), F32),
            pltpu.SemaphoreType.DMA((5,)),
            pltpu.SemaphoreType.DMA((7,)),
            pltpu.SemaphoreType.DMA((5, n_dev)),
            pltpu.SemaphoreType.DMA((5, n_dev)),
        ],
        compiler_params=pltpu.CompilerParams(collective_id=0, has_side_effects=True, vmem_limit_bytes=8 * MIB),
        name="front_pass",
    )(*[pltpu.with_memory_space_constraint(a, pltpu.HBM) for a in args])


def expert_kernel(n_dev, cap, pick_ref, d_ref, act_ref, fac1_ref, fac3_ref, wd_ref, wga_ref, wua_ref, wg_in, wu_in,
                  dwd_ref, dh1_ref, dh3_ref, *rest):
    part_refs = rest[:n_dev]
    wgb_ref, wub_ref, ret_ref, stage_ref, wdt_ref, wgt_ref, wut_ref, load_sem, out_sem = rest[n_dev:]
    n_loc = wd_ref.shape[0]
    n_stage = stage_ref.shape[0]
    n_turn = wut_ref.shape[2]
    me = lax.axis_index("ep")
    loads = {e: (pltpu.make_async_copy(wg_in.at[e], wgb_ref.at[e - SPLIT], load_sem.at[0, e - SPLIT]),
                 pltpu.make_async_copy(wu_in.at[e], wub_ref.at[e - SPLIT], load_sem.at[1, e - SPLIT]))
             for e in range(SPLIT, n_loc)}
    for e in loads:
        for cp in loads[e]:
            cp.start()
    outs = [pltpu.make_async_copy(stage_ref.at[e % n_stage], dwd_ref.at[e], out_sem.at[e % n_stage]) for e in range(n_loc)]

    def weights(e):
        return (wgb_ref[e - SPLIT], wub_ref[e - SPLIT]) if e in loads else (wga_ref[e], wua_ref[e])

    def turn_down(e):
        wdt_ref[e % 2] = wd_ref[e].T

    def turn_gate_up(e):
        if e in loads:
            for cp in loads[e]:
                cp.wait()
        wg, wu = weights(e)
        wgt_ref[e % 2] = wg.T
        wut_ref[e % 2] = wu[:n_turn].T

    def down_grad(e):
        if e >= n_stage:
            outs[e - n_stage].wait()
        stage_ref[e % n_stage] = dot(act_ref[e], d_ref[e], 0, 0)
        outs[e].start()

    def hidden_grad(e):
        grad_h = dot(d_ref[e], wd_ref[e], 1, 1) if e == 0 else dot(d_ref[e], wdt_ref[e % 2], 1, 0)
        grad_h = grad_h.astype(BF16).astype(F32)
        dh1_ref[e] = (grad_h * fac1_ref[e]).astype(BF16)
        dh3_ref[e] = (grad_h * fac3_ref[e]).astype(BF16)

    def row_grad(e):
        wg, wu = weights(e)
        if e == 0:
            ret = dot(dh1_ref[e], wg, 1, 1) + dot(dh3_ref[e], wu, 1, 1)
        else:
            up = [dot(dh3_ref[e], wut_ref[e % 2], 1, 0), dot(dh3_ref[e], wu[n_turn:], 1, 1)]
            ret = dot(dh1_ref[e], wgt_ref[e % 2], 1, 0) + jnp.concatenate(up, axis=1)
        ret = ret.astype(BF16)
        for s in range(n_dev):
            ret_ref[s, e * cap:(e + 1) * cap, :] = ret[s * cap:(s + 1) * cap, :]

    down_grad(0)
    hidden_grad(0)
    turn_down(1)
    for e in range(n_loc):
        if e + 1 < n_loc:
            down_grad(e + 1)
            hidden_grad(e + 1)
            turn_gate_up(e + 1)
        if e + 2 < n_loc:
            turn_down(e + 2)
        row_grad(e)
    for k in range(n_dev):
        part_refs[k][...] = dot(pick_ref[k], ret_ref[me ^ k], 0, 0)
    for e in range(n_loc - n_stage, n_loc):
        outs[e].wait()


def expert_pass(pick, d, act, fac1, fac3, wd, wga, wua, wg, wu, n_dev, cap):
    n_loc, ffn, model = wd.shape
    rows = d.shape[1]
    tok = pick.shape[2]
    n_stage = 2
    late = n_loc - SPLIT
    hbm = [pltpu.with_memory_space_constraint(a, pltpu.HBM) for a in (wg, wu)]
    return pl.pallas_call(
        functools.partial(expert_kernel, n_dev, cap),
        out_shape=[
            jax.ShapeDtypeStruct((n_loc, ffn, model), F32),
            pltpu.VMEM((n_loc, rows, ffn), BF16),
            pltpu.VMEM((n_loc, rows, ffn), BF16),
        ] + [pltpu.VMEM((tok, model), F32)] * n_dev,
        in_specs=[VMEM] * 8 + [ANY] * 2,
        out_specs=[ANY, VMEM, VMEM] + [VMEM] * n_dev,
        scratch_shapes=[
            pltpu.VMEM((late,) + wg.shape[1:], BF16),
            pltpu.VMEM((late,) + wu.shape[1:], BF16),
            pltpu.VMEM((n_dev, n_loc * cap, model), BF16),
            pltpu.VMEM((n_stage, ffn, model), F32),
            pltpu.VMEM((2, model, ffn), BF16),
            pltpu.VMEM((2, ffn, model), BF16),
            pltpu.VMEM((2, ffn, model // 2), BF16),
            pltpu.SemaphoreType.DMA((2, late)),
            pltpu.SemaphoreType.DMA((n_stage,)),
        ],
        compiler_params=pltpu.CompilerParams(vmem_limit_bytes=(15 + 2 * late) * MIB + MIB // 2),
        cost_estimate=pl.CostEstimate(flops=10 * n_loc * rows * ffn * model, bytes_accessed=50 * MIB, transcendentals=0),
        name="expert_pass",
    )(pick, d, act, fac1, fac3, wd, wga, wua, *hbm)


def weight_kernel(x_ref, dh1_ref, dh3_ref, gy_ref, y_ref, dwg_ref, dwu_ref, gg_ref, stage, gg_acc, gg_out, out_sem, gg_sem):
    n_loc, _, model = x_ref.shape
    top_k = y_ref.shape[1]
    half = model // 2
    gg_copy = pltpu.make_async_copy(gg_out, gg_ref, gg_sem)

    def out_copy(e, s, q):
        dst = (dwg_ref, dwu_ref)[q % 2].at[e, pl.ds(half * (q // 2), half), :]
        return pltpu.make_async_copy(stage.at[s, q], dst, out_sem.at[s, q])

    def one(e, s):
        for h in range(2):
            x = x_ref[e, :, h * half:(h + 1) * half]
            for w, dh in enumerate((dh1_ref, dh3_ref)):
                q = 2 * h + w
                stage[s, q] = dot(x, dh[e], 0, 0)
                out_copy(e, s, q).start()

    def wait_all(s):
        for q in range(4):
            out_copy(0, s, q).wait()

    def body(i, carry):
        for s in range(2):
            @pl.when(i > 0)
            def _():
                wait_all(s)
            one(2 * i + s, s)

        @pl.when(i == n_loc // 2 - 2)
        def _():
            step = 8
            for b in range(y_ref.shape[0] // step):
                prod = y_ref[b * step:(b + 1) * step].astype(F32) * gy_ref[0, b * step:(b + 1) * step].astype(F32)[:, None, :]
                gg_acc[b * step:(b + 1) * step, 0:top_k] = jnp.sum(prod, axis=2)
            gg_out[...] = gg_acc[...].T[0:top_k, :]
            gg_copy.start()
        return carry

    lax.fori_loop(0, n_loc // 2, body, 0)
    gg_copy.wait()
    wait_all(0)
    wait_all(1)


def weight_pass(x, dh1, dh3, gy, y):
    n_loc, rows, model = x.shape
    ffn = dh1.shape[2]
    tok, top_k, _ = y.shape
    grad_shape = jax.ShapeDtypeStruct((n_loc, model, ffn), F32)
    return pl.pallas_call(
        weight_kernel,
        out_shape=[grad_shape, grad_shape, jax.ShapeDtypeStruct((top_k, tok), F32)],
        in_specs=[VMEM] * 5,
        out_specs=[ANY, ANY, ANY],
        scratch_shapes=[
            pltpu.VMEM((2, 4, model // 2, ffn), F32),
            pltpu.VMEM((tok, 128), F32),
            pltpu.VMEM((top_k, tok), F32),
            pltpu.SemaphoreType.DMA((2, 4)),
            pltpu.SemaphoreType.DMA,
        ],
        compiler_params=pltpu.CompilerParams(vmem_limit_bytes=20 * MIB),
        cost_estimate=pl.CostEstimate(flops=4 * n_loc * rows * ffn * model, bytes_accessed=40 * MIB, transcendentals=0),
        name="weight_pass",
    )(x, dh1, dh3, gy, y)


def solution(mesh):
    n_dev = mesh.shape["ep"]
    rows_spec = P(("dp", "ep"), None)
    cube_spec = P(("dp", "ep"), None, None)
    weight_spec = P("ep", None, None)

    def local_step(grad_y, gate_vals, topk_idx, slot_ids, pair_counts, y_routed, x_disp, h_gate, h_up, w_gate, w_up, w_down):
        cap = x_disp.shape[1] // n_dev
        gy, pick, d, act, fac1, fac3, wd, wga, wua, x, y = front_pass(
            grad_y, topk_idx.T, slot_ids.T, gate_vals.T, pair_counts, h_gate, h_up, w_down, w_gate, w_up, x_disp, y_routed, n_dev, cap)
        dwd, dh1, dh3, *parts = expert_pass(pick, d, act, fac1, fac3, wd, wga, wua, w_gate, w_up, n_dev, cap)
        back = [lax.ppermute(parts[k], "ep", [(i, i ^ k) for i in range(n_dev)]) for k in range(1, n_dev)]
        dwg, dwu, gg = weight_pass(x, dh1, dh3, gy, y)
        total = parts[0]
        for b in back:
            total = total + b
        return total.astype(BF16), gg.T, dwg, dwu, dwd

    return jax.shard_map(local_step, mesh=mesh, in_specs=(rows_spec, rows_spec, rows_spec, rows_spec, rows_spec, cube_spec, cube_spec, cube_spec, cube_spec, weight_spec, weight_spec, weight_spec), out_specs=(rows_spec, rows_spec, cube_spec, cube_spec, cube_spec), check_vma=False)
```

```python
import functools

import jax
import jax.numpy as jnp
from jax import lax
from jax.experimental import pallas as pl
from jax.experimental.pallas import tpu as pltpu
from jax.sharding import PartitionSpec as P

MESH = pl.DeviceIdType.MESH
F32 = jnp.float32
BF16 = jnp.bfloat16
ANY = pl.BlockSpec(memory_space=pl.ANY)
VMEM = pl.BlockSpec(memory_space=pltpu.VMEM)
MIB = 2**20
SPLIT = 6
AHEAD = 3


def dot(a, b, ca, cb):
    return lax.dot_general(a, b, (((ca,), (cb,)), ((), ())), preferred_element_type=F32)


def front_kernel(n_dev, cap, gy_in, tk_in, sl_in, gt_in, ct_in, hg_in, hu_in, wd_in, wg_in, wu_in, x_in,
                 gy_ref, pick_ref, d_ref, act_ref, fac1_ref, fac3_ref, wd_ref, wg_ref, wu_ref, x_ref,
                 tk_ref, sl_ref, gt_ref, ct_ref, hg_ref, hu_ref, gate_ref, local_sem, load_sem, send_sem, recv_sem):
    me = lax.axis_index("ep")
    n_loc = d_ref.shape[0]
    bufs = [gy_ref, tk_ref, sl_ref, gt_ref, ct_ref]
    local = [pltpu.make_async_copy(a, b.at[0], local_sem.at[i])
             for i, (a, b) in enumerate(zip((gy_in, tk_in, sl_in, gt_in, ct_in), bufs))]
    pairs = [(hg_in, hg_ref), (hu_in, hu_ref), (wd_in, wd_ref), (wg_in.at[pl.ds(0, SPLIT)], wg_ref),
             (wu_in.at[pl.ds(0, SPLIT)], wu_ref), (x_in, x_ref)]
    loads = [pltpu.make_async_copy(a, b, load_sem.at[i]) for i, (a, b) in enumerate(pairs)]
    for cp in local:
        cp.start()
    barrier = pltpu.get_barrier_semaphore()
    for k in range(1, n_dev):
        pl.semaphore_signal(barrier, inc=1, device_id={"ep": me ^ k}, device_id_type=MESH)
    for cp in loads:
        cp.start()
    pl.semaphore_wait(barrier, n_dev - 1)
    for cp in local:
        cp.wait()

    def remote(i, k, src_slot, dst_slot):
        return pltpu.make_async_remote_copy(
            src_ref=bufs[i].at[src_slot], dst_ref=bufs[i].at[dst_slot],
            send_sem=send_sem.at[i, dst_slot], recv_sem=recv_sem.at[i, dst_slot],
            device_id={"ep": me ^ k}, device_id_type=MESH)

    far = remote(0, 2, 0, 2)
    near = remote(0, 1, 0, 1)
    relay = remote(0, 1, 2, 3)
    small = {k: [remote(i, k, 0, k) for i in range(1, len(bufs))] for k in range(1, n_dev)}
    for cp in small[2]:
        cp.start()
    far.start()
    for k in (3, 1):
        for cp in small[k]:
            cp.start()
    near.start()

    loads[0].wait()
    loads[1].wait()

    def silu(e, carry):
        gate_f = hg_ref[e].astype(F32)
        up_f = hu_ref[e].astype(F32)
        gate_sig = jax.nn.sigmoid(gate_f)
        gate_act = gate_f * gate_sig
        act_ref[e] = (gate_act * up_f).astype(BF16).T
        fac1_ref[e] = up_f * gate_sig * (1.0 + gate_f * (1.0 - gate_sig))
        fac3_ref[e] = gate_act
        return carry

    lax.fori_loop(0, n_loc, silu, 0)

    tok = tk_ref.shape[2]
    rows = n_loc * cap

    def select(k):
        row = lax.broadcasted_iota(jnp.int32, (rows, tok), 0) + me * rows
        key = jnp.where(sl_ref[k] >= 0, tk_ref[k] * cap + sl_ref[k], -1)
        gate = gt_ref[k]
        pick = jnp.zeros((rows, tok), F32)
        gate_sel = jnp.zeros((rows, tok), F32)
        for j in range(key.shape[0]):
            hit = key[j:j + 1, :] == row
            pick = jnp.where(hit, 1.0, pick)
            gate_sel = jnp.where(hit, gate[j:j + 1, :], gate_sel)
        row1 = lax.broadcasted_iota(jnp.int32, (rows, 1), 0)
        lane = lax.broadcasted_iota(jnp.int32, ct_ref.shape[1:], 1)
        count = jnp.zeros((rows, 1), jnp.int32)
        for e in range(n_loc):
            here = jnp.sum(jnp.where(lane == me * n_loc + e, ct_ref[k], 0), axis=1, keepdims=True)
            count = jnp.where(row1 // cap == e, here, count)
        pick_ref[k] = pick.astype(BF16)
        gate_ref[k] = jnp.where(row1 % cap < count, jnp.sum(gate_sel, axis=1, keepdims=True), 0.0)

    def gated_rows(k):
        rows_k = (dot(pick_ref[k], gy_ref[k], 1, 0) * gate_ref[k]).astype(BF16)
        at = pl.multiple_of((me ^ k) * cap, cap)
        for e in range(n_loc):
            d_ref[e, pl.ds(at, cap), :] = rows_k[e * cap:(e + 1) * cap, :]

    select(0)
    gated_rows(0)
    for k in (1, 2, 3):
        for cp in small[k]:
            cp.wait()
        select(k)
    near.wait()
    gated_rows(1)
    far.wait_recv()
    relay.start()
    gated_rows(2)
    relay.wait()
    gated_rows(3)
    far.wait_send()
    for cp in loads[2:]:
        cp.wait()


def front_pass(gy, tk, sl, gt, ct, hg, hu, wd, wg, wu, x, n_dev, cap):
    args = (gy, tk, sl, gt, ct, hg, hu, wd, wg, wu, x)
    n_loc, ffn, model = wd.shape
    tok = gy.shape[0]
    rows = hg.shape[1]
    outs = [
        pltpu.VMEM((n_dev, tok, model), BF16),
        pltpu.VMEM((n_dev, n_loc * cap, tok), BF16),
        pltpu.VMEM((n_loc, rows, model), BF16),
        pltpu.VMEM((n_loc, ffn, rows), BF16),
        pltpu.VMEM((n_loc, rows, ffn), F32),
        pltpu.VMEM((n_loc, rows, ffn), F32),
        pltpu.VMEM(wd.shape, BF16),
        pltpu.VMEM((SPLIT,) + wg.shape[1:], BF16),
        pltpu.VMEM((SPLIT,) + wu.shape[1:], BF16),
        pltpu.VMEM(x.shape, BF16),
    ]
    return pl.pallas_call(
        functools.partial(front_kernel, n_dev, cap),
        out_shape=outs,
        in_specs=[ANY] * len(args),
        out_specs=[VMEM] * len(outs),
        scratch_shapes=[
            pltpu.VMEM((n_dev,) + tk.shape, jnp.int32),
            pltpu.VMEM((n_dev,) + sl.shape, jnp.int32),
            pltpu.VMEM((n_dev,) + gt.shape, F32),
            pltpu.VMEM((n_dev,) + ct.shape, jnp.int32),
            pltpu.VMEM(hg.shape, BF16),
            pltpu.VMEM(hu.shape, BF16),
            pltpu.VMEM((n_dev, n_loc * cap, 1), F32),
            pltpu.SemaphoreType.DMA((5,)),
            pltpu.SemaphoreType.DMA((6,)),
            pltpu.SemaphoreType.DMA((5, n_dev)),
            pltpu.SemaphoreType.DMA((5, n_dev)),
        ],
        compiler_params=pltpu.CompilerParams(collective_id=0, has_side_effects=True, vmem_limit_bytes=5 * MIB),
        name="front_pass",
    )(*[pltpu.with_memory_space_constraint(a, pltpu.HBM) for a in args])


def expert_kernel(n_dev, cap, pick_ref, d_ref, act_ref, fac1_ref, fac3_ref, wd_ref, wga_ref, wua_ref, wg_in, wu_in,
                  dwd_ref, dh1_ref, dh3_ref, *rest):
    part_refs = rest[:n_dev]
    wgb_ref, wub_ref, ret_ref, stage_ref, wdt_ref, wgt_ref, wut_ref, load_sem, out_sem = rest[n_dev:]
    n_loc = wd_ref.shape[0]
    n_stage = stage_ref.shape[0]
    n_turn = wut_ref.shape[2]
    me = lax.axis_index("ep")
    loads = {e: (pltpu.make_async_copy(wg_in.at[e], wgb_ref.at[e - SPLIT], load_sem.at[0, e - SPLIT]),
                 pltpu.make_async_copy(wu_in.at[e], wub_ref.at[e - SPLIT], load_sem.at[1, e - SPLIT]))
             for e in range(SPLIT, n_loc)}
    outs = [pltpu.make_async_copy(stage_ref.at[e % n_stage], dwd_ref.at[e], out_sem.at[e % n_stage]) for e in range(n_loc)]

    def weights(e):
        return (wgb_ref[e - SPLIT], wub_ref[e - SPLIT]) if e in loads else (wga_ref[e], wua_ref[e])

    def turn_down(e):
        wdt_ref[e % 2] = wd_ref[e].T

    def turn_gate_up(e):
        if e in loads:
            for cp in loads[e]:
                cp.wait()
        wg, wu = weights(e)
        wgt_ref[e % 2] = wg.T
        wut_ref[e % 2] = wu[:n_turn].T

    def down_grad(e):
        if e >= n_stage:
            outs[e - n_stage].wait()
        stage_ref[e % n_stage] = dot(act_ref[e], d_ref[e], 1, 0)
        outs[e].start()

    def hidden_grad(e):
        grad_h = dot(d_ref[e], wd_ref[e], 1, 1) if e == 0 else dot(d_ref[e], wdt_ref[e % 2], 1, 0)
        grad_h = grad_h.astype(BF16).astype(F32)
        dh1_ref[e] = (grad_h * fac1_ref[e]).astype(BF16)
        dh3_ref[e] = (grad_h * fac3_ref[e]).astype(BF16)

    def row_grad(e):
        wg, wu = weights(e)
        if e == 0:
            ret = dot(dh1_ref[e], wg, 1, 1) + dot(dh3_ref[e], wu, 1, 1)
        else:
            up = [dot(dh3_ref[e], wut_ref[e % 2], 1, 0), dot(dh3_ref[e], wu[n_turn:], 1, 1)]
            ret = dot(dh1_ref[e], wgt_ref[e % 2], 1, 0) + jnp.concatenate(up, axis=1)
        ret = ret.astype(BF16)
        for s in range(n_dev):
            ret_ref[s, e * cap:(e + 1) * cap, :] = ret[s * cap:(s + 1) * cap, :]

    down_grad(0)
    hidden_grad(0)
    turn_down(1)
    for e in range(n_loc):
        if e + AHEAD in loads:
            for cp in loads[e + AHEAD]:
                cp.start()
        if e + 1 < n_loc:
            down_grad(e + 1)
            hidden_grad(e + 1)
            turn_gate_up(e + 1)
        if e + 2 < n_loc:
            turn_down(e + 2)
        row_grad(e)
    for k in range(n_dev):
        part_refs[k][...] = dot(pick_ref[k], ret_ref[me ^ k], 0, 0)
    for e in range(n_loc - n_stage, n_loc):
        outs[e].wait()


def expert_pass(pick, d, act, fac1, fac3, wd, wga, wua, wg, wu, n_dev, cap):
    n_loc, ffn, model = wd.shape
    rows = d.shape[1]
    tok = pick.shape[2]
    n_stage = 4
    late = n_loc - SPLIT
    hbm = [pltpu.with_memory_space_constraint(a, pltpu.HBM) for a in (wg, wu)]
    return pl.pallas_call(
        functools.partial(expert_kernel, n_dev, cap),
        out_shape=[
            jax.ShapeDtypeStruct((n_loc, ffn, model), F32),
            pltpu.VMEM((n_loc, rows, ffn), BF16),
            pltpu.VMEM((n_loc, rows, ffn), BF16),
        ] + [pltpu.VMEM((tok, model), F32)] * n_dev,
        in_specs=[VMEM] * 8 + [ANY] * 2,
        out_specs=[ANY, VMEM, VMEM] + [VMEM] * n_dev,
        scratch_shapes=[
            pltpu.VMEM((late,) + wg.shape[1:], BF16),
            pltpu.VMEM((late,) + wu.shape[1:], BF16),
            pltpu.VMEM((n_dev, n_loc * cap, model), BF16),
            pltpu.VMEM((n_stage, ffn, model), F32),
            pltpu.VMEM((2, model, ffn), BF16),
            pltpu.VMEM((2, ffn, model), BF16),
            pltpu.VMEM((2, ffn, model // 2), BF16),
            pltpu.SemaphoreType.DMA((2, late)),
            pltpu.SemaphoreType.DMA((n_stage,)),
        ],
        compiler_params=pltpu.CompilerParams(vmem_limit_bytes=(16 + 2 * late) * MIB),
        cost_estimate=pl.CostEstimate(flops=10 * n_loc * rows * ffn * model, bytes_accessed=50 * MIB, transcendentals=0),
        name="expert_pass",
    )(pick, d, act, fac1, fac3, wd, wga, wua, *hbm)


def weight_kernel(x_ref, dh1_ref, dh3_ref, gy_ref, y_in, dwg_ref, dwu_ref, gg_ref, y_ref, stage, gg_acc, gg_out, out_sem, gg_sem):
    n_loc, _, model = x_ref.shape
    top_k = y_ref.shape[1]
    half = model // 2
    gg_copy = pltpu.make_async_copy(gg_out, gg_ref, gg_sem.at[0])
    y_copy = pltpu.make_async_copy(y_in, y_ref, gg_sem.at[1])
    y_copy.start()

    def out_copy(e, s, q):
        dst = (dwg_ref, dwu_ref)[q % 2].at[e, pl.ds(half * (q // 2), half), :]
        return pltpu.make_async_copy(stage.at[s, q], dst, out_sem.at[s, q])

    def one(e, s):
        for h in range(2):
            x = x_ref[e, :, h * half:(h + 1) * half]
            for w, dh in enumerate((dh1_ref, dh3_ref)):
                q = 2 * h + w
                stage[s, q] = dot(x, dh[e], 0, 0)
                out_copy(e, s, q).start()

    def wait_all(s):
        for q in range(4):
            out_copy(0, s, q).wait()

    def body(i, carry):
        for s in range(2):
            @pl.when(i > 0)
            def _():
                wait_all(s)
            one(2 * i + s, s)

        @pl.when(i == n_loc // 2 - 2)
        def _():
            y_copy.wait()
            step = 8
            for b in range(y_ref.shape[0] // step):
                prod = y_ref[b * step:(b + 1) * step].astype(F32) * gy_ref[0, b * step:(b + 1) * step].astype(F32)[:, None, :]
                gg_acc[b * step:(b + 1) * step, 0:top_k] = jnp.sum(prod, axis=2)
            gg_out[...] = gg_acc[...].T[0:top_k, :]
            gg_copy.start()
        return carry

    lax.fori_loop(0, n_loc // 2, body, 0)
    gg_copy.wait()
    wait_all(0)
    wait_all(1)


def weight_pass(x, dh1, dh3, gy, y):
    n_loc, rows, model = x.shape
    ffn = dh1.shape[2]
    tok, top_k, _ = y.shape
    grad_shape = jax.ShapeDtypeStruct((n_loc, model, ffn), F32)
    return pl.pallas_call(
        weight_kernel,
        out_shape=[grad_shape, grad_shape, jax.ShapeDtypeStruct((top_k, tok), F32)],
        in_specs=[VMEM] * 4 + [ANY],
        out_specs=[ANY, ANY, ANY],
        scratch_shapes=[
            pltpu.VMEM(y.shape, BF16),
            pltpu.VMEM((2, 4, model // 2, ffn), F32),
            pltpu.VMEM((tok, 128), F32),
            pltpu.VMEM((top_k, tok), F32),
            pltpu.SemaphoreType.DMA((2, 4)),
            pltpu.SemaphoreType.DMA((2,)),
        ],
        compiler_params=pltpu.CompilerParams(vmem_limit_bytes=20 * MIB),
        cost_estimate=pl.CostEstimate(flops=4 * n_loc * rows * ffn * model, bytes_accessed=40 * MIB, transcendentals=0),
        name="weight_pass",
    )(x, dh1, dh3, gy, pltpu.with_memory_space_constraint(y, pltpu.HBM))


def solution(mesh):
    n_dev = mesh.shape["ep"]
    rows_spec = P(("dp", "ep"), None)
    cube_spec = P(("dp", "ep"), None, None)
    weight_spec = P("ep", None, None)

    def local_step(grad_y, gate_vals, topk_idx, slot_ids, pair_counts, y_routed, x_disp, h_gate, h_up, w_gate, w_up, w_down):
        cap = x_disp.shape[1] // n_dev
        gy, pick, d, act, fac1, fac3, wd, wga, wua, x = front_pass(
            grad_y, topk_idx.T, slot_ids.T, gate_vals.T, pair_counts, h_gate, h_up, w_down, w_gate, w_up, x_disp, n_dev, cap)
        dwd, dh1, dh3, *parts = expert_pass(pick, d, act, fac1, fac3, wd, wga, wua, w_gate, w_up, n_dev, cap)
        back = [lax.ppermute(parts[k], "ep", [(i, i ^ k) for i in range(n_dev)]) for k in range(1, n_dev)]
        dwg, dwu, gg = weight_pass(x, dh1, dh3, gy, y_routed)
        total = parts[0]
        for b in back:
            total = total + b
        return total.astype(BF16), gg.T, dwg, dwu, dwd

    return jax.shard_map(local_step, mesh=mesh, in_specs=(rows_spec, rows_spec, rows_spec, rows_spec, rows_spec, cube_spec, cube_spec, cube_spec, cube_spec, weight_spec, weight_spec, weight_spec), out_specs=(rows_spec, rows_spec, cube_spec, cube_spec, cube_spec), check_vma=False)
```

```python
import functools

import jax
import jax.numpy as jnp
from jax import lax
from jax.experimental import pallas as pl
from jax.experimental.pallas import tpu as pltpu
from jax.sharding import PartitionSpec as P

MESH = pl.DeviceIdType.MESH
F32 = jnp.float32
BF16 = jnp.bfloat16
ANY = pl.BlockSpec(memory_space=pl.ANY)
VMEM = pl.BlockSpec(memory_space=pltpu.VMEM)
MIB = 2**20
SPLIT = 6
AHEAD = 3
LEAD = 2


def dot(a, b, ca, cb):
    return lax.dot_general(a, b, (((ca,), (cb,)), ((), ())), preferred_element_type=F32)


def front_kernel(n_dev, cap, gy_in, tk_in, sl_in, gt_in, ct_in, hg_in, hu_in, wd_in, wg_in, wu_in,
                 gy_ref, pick_ref, d_ref, act_ref, fac1_ref, fac3_ref, wd_ref, wg_ref, wu_ref,
                 tk_ref, sl_ref, gt_ref, ct_ref, hg_ref, hu_ref, gate_ref, local_sem, load_sem, send_sem, recv_sem):
    me = lax.axis_index("ep")
    n_loc = d_ref.shape[0]
    bufs = [gy_ref, tk_ref, sl_ref, gt_ref, ct_ref]
    ins = [gy_in, tk_in, sl_in, gt_in, ct_in]
    local = [pltpu.make_async_copy(a, b.at[0], local_sem.at[i])
             for i, (a, b) in enumerate(zip((gy_in, tk_in, sl_in, gt_in, ct_in), bufs))]
    pairs = [(hg_in, hg_ref), (hu_in, hu_ref), (wd_in, wd_ref), (wg_in.at[pl.ds(0, SPLIT)], wg_ref),
             (wu_in.at[pl.ds(0, SPLIT)], wu_ref)]
    loads = [pltpu.make_async_copy(a, b, load_sem.at[i]) for i, (a, b) in enumerate(pairs)]
    for cp in local:
        cp.start()
    barrier = pltpu.get_barrier_semaphore()
    for k in range(1, n_dev):
        pl.semaphore_signal(barrier, inc=1, device_id={"ep": me ^ k}, device_id_type=MESH)
    for cp in loads:
        cp.start()
    pl.semaphore_wait(barrier, n_dev - 1)

    def remote(i, k, src_slot, dst_slot):
        return pltpu.make_async_remote_copy(
            src_ref=bufs[i].at[src_slot] if src_slot else ins[i], dst_ref=bufs[i].at[dst_slot],
            send_sem=send_sem.at[i, dst_slot], recv_sem=recv_sem.at[i, dst_slot],
            device_id={"ep": me ^ k}, device_id_type=MESH)

    far = remote(0, 2, 0, 2)
    near = remote(0, 1, 0, 1)
    relay = remote(0, 1, 2, 3)
    small = {k: [remote(i, k, 0, k) for i in range(1, len(bufs))] for k in range(1, n_dev)}
    for cp in small[2]:
        cp.start()
    far.start()
    for k in (3, 1):
        for cp in small[k]:
            cp.start()
    near.start()

    for cp in local:
        cp.wait()
    loads[0].wait()
    loads[1].wait()

    def silu(e, carry):
        gate_f = hg_ref[e].astype(F32)
        up_f = hu_ref[e].astype(F32)
        gate_sig = jax.nn.sigmoid(gate_f)
        gate_act = gate_f * gate_sig
        act_ref[e] = (gate_act * up_f).astype(BF16).T
        fac1_ref[e] = up_f * gate_sig * (1.0 + gate_f * (1.0 - gate_sig))
        fac3_ref[e] = gate_act
        return carry

    lax.fori_loop(0, n_loc, silu, 0)

    tok = tk_ref.shape[2]
    rows = n_loc * cap

    def select(k):
        row = lax.broadcasted_iota(jnp.int32, (rows, tok), 0) + me * rows
        key = jnp.where(sl_ref[k] >= 0, tk_ref[k] * cap + sl_ref[k], -1)
        gate = gt_ref[k]
        pick = jnp.zeros((rows, tok), F32)
        gate_sel = jnp.zeros((rows, tok), F32)
        for j in range(key.shape[0]):
            hit = key[j:j + 1, :] == row
            pick = jnp.where(hit, 1.0, pick)
            gate_sel = jnp.where(hit, gate[j:j + 1, :], gate_sel)
        row1 = lax.broadcasted_iota(jnp.int32, (rows, 1), 0)
        lane = lax.broadcasted_iota(jnp.int32, ct_ref.shape[1:], 1)
        count = jnp.zeros((rows, 1), jnp.int32)
        for e in range(n_loc):
            here = jnp.sum(jnp.where(lane == me * n_loc + e, ct_ref[k], 0), axis=1, keepdims=True)
            count = jnp.where(row1 // cap == e, here, count)
        pick_ref[k] = pick.astype(BF16)
        gate_ref[k] = jnp.where(row1 % cap < count, jnp.sum(gate_sel, axis=1, keepdims=True), 0.0)

    def gated_rows(k):
        rows_k = (dot(pick_ref[k], gy_ref[k], 1, 0) * gate_ref[k]).astype(BF16)
        at = pl.multiple_of((me ^ k) * cap, cap)
        for e in range(n_loc):
            d_ref[e, pl.ds(at, cap), :] = rows_k[e * cap:(e + 1) * cap, :]

    select(0)
    gated_rows(0)
    for k in (1, 2, 3):
        for cp in small[k]:
            cp.wait()
        select(k)
    near.wait()
    gated_rows(1)
    far.wait_recv()
    relay.start()
    gated_rows(2)
    relay.wait()
    gated_rows(3)
    far.wait_send()
    for cp in loads[2:]:
        cp.wait()


def front_pass(gy, tk, sl, gt, ct, hg, hu, wd, wg, wu, n_dev, cap):
    args = (gy, tk, sl, gt, ct, hg, hu, wd, wg, wu)
    n_loc, ffn, model = wd.shape
    tok = gy.shape[0]
    rows = hg.shape[1]
    outs = [
        pltpu.VMEM((n_dev, tok, model), BF16),
        pltpu.VMEM((n_dev, n_loc * cap, tok), BF16),
        pltpu.VMEM((n_loc, rows, model), BF16),
        pltpu.VMEM((n_loc, ffn, rows), BF16),
        pltpu.VMEM((n_loc, rows, ffn), F32),
        pltpu.VMEM((n_loc, rows, ffn), F32),
        pltpu.VMEM(wd.shape, BF16),
        pltpu.VMEM((SPLIT,) + wg.shape[1:], BF16),
        pltpu.VMEM((SPLIT,) + wu.shape[1:], BF16),
    ]
    return pl.pallas_call(
        functools.partial(front_kernel, n_dev, cap),
        out_shape=outs,
        in_specs=[ANY] * len(args),
        out_specs=[VMEM] * len(outs),
        scratch_shapes=[
            pltpu.VMEM((n_dev,) + tk.shape, jnp.int32),
            pltpu.VMEM((n_dev,) + sl.shape, jnp.int32),
            pltpu.VMEM((n_dev,) + gt.shape, F32),
            pltpu.VMEM((n_dev,) + ct.shape, jnp.int32),
            pltpu.VMEM(hg.shape, BF16),
            pltpu.VMEM(hu.shape, BF16),
            pltpu.VMEM((n_dev, n_loc * cap, 1), F32),
            pltpu.SemaphoreType.DMA((5,)),
            pltpu.SemaphoreType.DMA((5,)),
            pltpu.SemaphoreType.DMA((5, n_dev)),
            pltpu.SemaphoreType.DMA((5, n_dev)),
        ],
        compiler_params=pltpu.CompilerParams(collective_id=0, has_side_effects=True, vmem_limit_bytes=4 * MIB),
        name="front_pass",
    )(*[pltpu.with_memory_space_constraint(a, pltpu.HBM) for a in args])


def expert_kernel(n_dev, cap, pick_ref, d_ref, act_ref, fac1_ref, fac3_ref, wd_ref, wga_ref, wua_ref, wg_in, wu_in,
                  dwd_ref, dh1_ref, dh3_ref, *rest):
    part_refs = rest[:n_dev]
    wgb_ref, wub_ref, ret_ref, stage_ref, wdt_ref, wgt_ref, wut_ref, load_sem, out_sem = rest[n_dev:]
    n_loc = wd_ref.shape[0]
    n_stage = stage_ref.shape[0]
    n_turn = wut_ref.shape[2]
    me = lax.axis_index("ep")
    loads = {e: (pltpu.make_async_copy(wg_in.at[e], wgb_ref.at[e - SPLIT], load_sem.at[0, e - SPLIT]),
                 pltpu.make_async_copy(wu_in.at[e], wub_ref.at[e - SPLIT], load_sem.at[1, e - SPLIT]))
             for e in range(SPLIT, n_loc)}
    outs = [pltpu.make_async_copy(stage_ref.at[e % n_stage], dwd_ref.at[e], out_sem.at[e % n_stage]) for e in range(n_loc)]

    def weights(e):
        return (wgb_ref[e - SPLIT], wub_ref[e - SPLIT]) if e in loads else (wga_ref[e], wua_ref[e])

    def turn_down(e):
        wdt_ref[e % 2] = wd_ref[e].T

    def turn_gate_up(e):
        wg, wu = weights(e)
        wgt_ref[e % 2] = wg.T
        wut_ref[e % 2] = wu[:n_turn].T

    def down_grad(e):
        stage_ref[e % n_stage] = dot(act_ref[e], d_ref[e], 1, 0)

    def hidden_grad(e):
        grad_h = dot(d_ref[e], wd_ref[e], 1, 1) if e == 0 else dot(d_ref[e], wdt_ref[e % 2], 1, 0)
        grad_h = grad_h.astype(BF16).astype(F32)
        dh1_ref[e] = (grad_h * fac1_ref[e]).astype(BF16)
        dh3_ref[e] = (grad_h * fac3_ref[e]).astype(BF16)

    def row_grad(e):
        wg, wu = weights(e)
        if e == 0:
            ret = dot(dh1_ref[e], wg, 1, 1) + dot(dh3_ref[e], wu, 1, 1)
        else:
            up = [dot(dh3_ref[e], wut_ref[e % 2], 1, 0), dot(dh3_ref[e], wu[n_turn:], 1, 1)]
            ret = dot(dh1_ref[e], wgt_ref[e % 2], 1, 0) + jnp.concatenate(up, axis=1)
        ret = ret.astype(BF16)
        for s in range(n_dev):
            ret_ref[s, e * cap:(e + 1) * cap, :] = ret[s * cap:(s + 1) * cap, :]

    for e in range(LEAD):
        down_grad(e)
    hidden_grad(0)
    turn_down(1)
    for e in range(0, n_loc, 2):
        for b in (e, e + 1):
            if b < n_loc and b < LEAD + e:
                outs[b].start()
        for b in (e + AHEAD, e + AHEAD + 1):
            if b in loads:
                for cp in loads[b]:
                    cp.start()
        for b in (e + LEAD, e + LEAD + 1):
            if b < n_loc and b >= n_stage:
                outs[b - n_stage].wait()
        for b in (e + 1, e + 2):
            if b in loads:
                for cp in loads[b]:
                    cp.wait()
        for f in (e, e + 1):
            if f + LEAD < n_loc:
                down_grad(f + LEAD)
            if f + 1 < n_loc:
                hidden_grad(f + 1)
                turn_gate_up(f + 1)
            if f + 2 < n_loc:
                turn_down(f + 2)
            row_grad(f)
    for k in range(n_dev):
        part_refs[k][...] = dot(pick_ref[k], ret_ref[me ^ k], 0, 0)
    for e in range(n_loc - n_stage, n_loc):
        outs[e].wait()


def expert_pass(pick, d, act, fac1, fac3, wd, wga, wua, wg, wu, n_dev, cap):
    n_loc, ffn, model = wd.shape
    rows = d.shape[1]
    tok = pick.shape[2]
    n_stage = 4
    late = n_loc - SPLIT
    hbm = [pltpu.with_memory_space_constraint(a, pltpu.HBM) for a in (wg, wu)]
    return pl.pallas_call(
        functools.partial(expert_kernel, n_dev, cap),
        out_shape=[
            jax.ShapeDtypeStruct((n_loc, ffn, model), F32),
            pltpu.VMEM((n_loc, rows, ffn), BF16),
            pltpu.VMEM((n_loc, rows, ffn), BF16),
        ] + [pltpu.VMEM((tok, model), F32)] * n_dev,
        in_specs=[VMEM] * 8 + [ANY] * 2,
        out_specs=[ANY, VMEM, VMEM] + [VMEM] * n_dev,
        scratch_shapes=[
            pltpu.VMEM((late,) + wg.shape[1:], BF16),
            pltpu.VMEM((late,) + wu.shape[1:], BF16),
            pltpu.VMEM((n_dev, n_loc * cap, model), BF16),
            pltpu.VMEM((n_stage, ffn, model), F32),
            pltpu.VMEM((2, model, ffn), BF16),
            pltpu.VMEM((2, ffn, model), BF16),
            pltpu.VMEM((2, ffn, model // 2), BF16),
            pltpu.SemaphoreType.DMA((2, late)),
            pltpu.SemaphoreType.DMA((n_stage,)),
        ],
        compiler_params=pltpu.CompilerParams(vmem_limit_bytes=(16 + 2 * late) * MIB),
        cost_estimate=pl.CostEstimate(flops=10 * n_loc * rows * ffn * model, bytes_accessed=50 * MIB, transcendentals=0),
        name="expert_pass",
    )(pick, d, act, fac1, fac3, wd, wga, wua, *hbm)


def weight_kernel(x_ref, dh1_ref, dh3_ref, gy_ref, y_in, dwg_ref, dwu_ref, gg_ref, y_ref, stage, gg_acc, gg_out, out_sem, gg_sem):
    n_loc, _, model = x_ref.shape
    top_k = y_ref.shape[1]
    half = model // 2
    gg_copy = pltpu.make_async_copy(gg_out, gg_ref, gg_sem.at[0])
    y_copy = pltpu.make_async_copy(y_in, y_ref, gg_sem.at[1])
    y_copy.start()

    def out_copy(e, s, q):
        dst = (dwg_ref, dwu_ref)[q % 2].at[e, pl.ds(half * (q // 2), half), :]
        return pltpu.make_async_copy(stage.at[s, q], dst, out_sem.at[s, q])

    def one(e, s):
        for h in range(2):
            x = x_ref[e, :, h * half:(h + 1) * half]
            for w, dh in enumerate((dh1_ref, dh3_ref)):
                q = 2 * h + w
                stage[s, q] = dot(x, dh[e], 0, 0)
                out_copy(e, s, q).start()

    def wait_all(s):
        for q in range(4):
            out_copy(0, s, q).wait()

    def body(i, carry):
        for s in range(2):
            @pl.when(i > 0)
            def _():
                wait_all(s)
            one(2 * i + s, s)

        @pl.when(i == n_loc // 2 - 2)
        def _():
            y_copy.wait()
            step = 8
            for b in range(y_ref.shape[0] // step):
                prod = y_ref[b * step:(b + 1) * step].astype(F32) * gy_ref[0, b * step:(b + 1) * step].astype(F32)[:, None, :]
                gg_acc[b * step:(b + 1) * step, 0:top_k] = jnp.sum(prod, axis=2)
            gg_out[...] = gg_acc[...].T[0:top_k, :]
            gg_copy.start()
        return carry

    lax.fori_loop(0, n_loc // 2, body, 0)
    gg_copy.wait()
    wait_all(0)
    wait_all(1)


def weight_pass(x, dh1, dh3, gy, y):
    n_loc, rows, model = x.shape
    ffn = dh1.shape[2]
    tok, top_k, _ = y.shape
    grad_shape = jax.ShapeDtypeStruct((n_loc, model, ffn), F32)
    return pl.pallas_call(
        weight_kernel,
        out_shape=[grad_shape, grad_shape, jax.ShapeDtypeStruct((top_k, tok), F32)],
        in_specs=[VMEM] * 4 + [ANY],
        out_specs=[ANY, ANY, ANY],
        scratch_shapes=[
            pltpu.VMEM(y.shape, BF16),
            pltpu.VMEM((2, 4, model // 2, ffn), F32),
            pltpu.VMEM((tok, 128), F32),
            pltpu.VMEM((top_k, tok), F32),
            pltpu.SemaphoreType.DMA((2, 4)),
            pltpu.SemaphoreType.DMA((2,)),
        ],
        compiler_params=pltpu.CompilerParams(vmem_limit_bytes=11 * MIB),
        cost_estimate=pl.CostEstimate(flops=4 * n_loc * rows * ffn * model, bytes_accessed=40 * MIB, transcendentals=0),
        name="weight_pass",
    )(x, dh1, dh3, gy, pltpu.with_memory_space_constraint(y, pltpu.HBM))


def solution(mesh):
    n_dev = mesh.shape["ep"]
    rows_spec = P(("dp", "ep"), None)
    cube_spec = P(("dp", "ep"), None, None)
    weight_spec = P("ep", None, None)

    def local_step(grad_y, gate_vals, topk_idx, slot_ids, pair_counts, y_routed, x_disp, h_gate, h_up, w_gate, w_up, w_down):
        cap = x_disp.shape[1] // n_dev
        gy, pick, d, act, fac1, fac3, wd, wga, wua = front_pass(
            grad_y, topk_idx.T, slot_ids.T, gate_vals.T, pair_counts, h_gate, h_up, w_down, w_gate, w_up, n_dev, cap)
        dwd, dh1, dh3, *parts = expert_pass(pick, d, act, fac1, fac3, wd, wga, wua, w_gate, w_up, n_dev, cap)
        back = [lax.ppermute(parts[k], "ep", [(i, i ^ k) for i in range(n_dev)]) for k in (2, 3, 1)]
        x, _ = lax.optimization_barrier((x_disp, parts[0]))
        dwg, dwu, gg = weight_pass(x, dh1, dh3, gy, y_routed)
        total = parts[0]
        for b in back:
            total = total + b
        return total.astype(BF16), gg.T, dwg, dwu, dwd

    return jax.shard_map(local_step, mesh=mesh, in_specs=(rows_spec, rows_spec, rows_spec, rows_spec, rows_spec, cube_spec, cube_spec, cube_spec, cube_spec, weight_spec, weight_spec, weight_spec), out_specs=(rows_spec, rows_spec, cube_spec, cube_spec, cube_spec), check_vma=False)
```

```python
import functools

import jax
import jax.numpy as jnp
from jax import lax
from jax.experimental import pallas as pl
from jax.experimental.pallas import tpu as pltpu
from jax.sharding import PartitionSpec as P

MESH = pl.DeviceIdType.MESH
F32 = jnp.float32
BF16 = jnp.bfloat16
ANY = pl.BlockSpec(memory_space=pl.ANY)
VMEM = pl.BlockSpec(memory_space=pltpu.VMEM)
MIB = 2**20
SPLIT = 6
AHEAD = 3
DIRECT = 16
LEAD = 2


def dot(a, b, ca, cb):
    return lax.dot_general(a, b, (((ca,), (cb,)), ((), ())), preferred_element_type=F32)


def front_kernel(n_dev, cap, gy_in, tk_in, sl_in, gt_in, ct_in, hg_in, hu_in, wd_in, wg_in, wu_in,
                 gy_ref, pick_ref, d_ref, act_ref, fac1_ref, fac3_ref, wd_ref, wg_ref, wu_ref,
                 tk_ref, sl_ref, gt_ref, ct_ref, hg_ref, hu_ref, gate_ref, local_sem, load_sem, send_sem, recv_sem, piece_send, piece_recv):
    me = lax.axis_index("ep")
    n_loc = d_ref.shape[0]
    bufs = [gy_ref, tk_ref, sl_ref, gt_ref, ct_ref]
    ins = [gy_in, tk_in, sl_in, gt_in, ct_in]
    local = [pltpu.make_async_copy(a, b.at[0], local_sem.at[i])
             for i, (a, b) in enumerate(zip((gy_in, tk_in, sl_in, gt_in, ct_in), bufs))]
    pairs = [(hg_in, hg_ref), (hu_in, hu_ref), (wd_in, wd_ref), (wg_in.at[pl.ds(0, SPLIT)], wg_ref),
             (wu_in.at[pl.ds(0, SPLIT)], wu_ref)]
    loads = [pltpu.make_async_copy(a, b, load_sem.at[i]) for i, (a, b) in enumerate(pairs)]
    for cp in local:
        cp.start()
    barrier = pltpu.get_barrier_semaphore()
    for k in range(1, n_dev):
        pl.semaphore_signal(barrier, inc=1, device_id={"ep": me ^ k}, device_id_type=MESH)
    for cp in loads:
        cp.start()
    pl.semaphore_wait(barrier, n_dev - 1)

    def remote(i, k):
        return pltpu.make_async_remote_copy(
            src_ref=ins[i], dst_ref=bufs[i].at[k], send_sem=send_sem.at[i, k], recv_sem=recv_sem.at[i, k],
            device_id={"ep": me ^ k}, device_id_type=MESH)

    def piece(n, k, src, slot, at, size):
        return pltpu.make_async_remote_copy(
            src_ref=src.at[pl.ds(at, size)], dst_ref=gy_ref.at[slot, pl.ds(at, size)],
            send_sem=piece_send.at[n], recv_sem=piece_recv.at[n], device_id={"ep": me ^ k}, device_id_type=MESH)

    tok = gy_in.shape[0]
    head = tok - DIRECT
    far_head = piece(0, 2, gy_in, 2, 0, head)
    far_tail = piece(1, 2, gy_in, 2, head, DIRECT)
    cross_tail = piece(2, 3, gy_in, 3, head, DIRECT)
    relay_head = piece(3, 1, gy_ref.at[2], 3, 0, head)
    near = remote(0, 1)
    small = {k: [remote(i, k) for i in range(1, len(bufs))] for k in range(1, n_dev)}
    for k in (2, 3):
        for cp in small[k]:
            cp.start()
    far_head.start()
    far_tail.start()
    cross_tail.start()
    for cp in small[1]:
        cp.start()
    near.start()

    for cp in local:
        cp.wait()
    loads[0].wait()
    loads[1].wait()

    def silu(e, carry):
        gate_f = hg_ref[e].astype(F32)
        up_f = hu_ref[e].astype(F32)
        gate_sig = jax.nn.sigmoid(gate_f)
        gate_act = gate_f * gate_sig
        act_ref[e] = (gate_act * up_f).astype(BF16).T
        fac1_ref[e] = up_f * gate_sig * (1.0 + gate_f * (1.0 - gate_sig))
        fac3_ref[e] = gate_act
        return carry

    lax.fori_loop(0, n_loc, silu, 0)

    rows = n_loc * cap

    def select(k):
        row = lax.broadcasted_iota(jnp.int32, (rows, tok), 0) + me * rows
        key = jnp.where(sl_ref[k] >= 0, tk_ref[k] * cap + sl_ref[k], -1)
        gate = gt_ref[k]
        pick = jnp.zeros((rows, tok), F32)
        gate_sel = jnp.zeros((rows, tok), F32)
        for j in range(key.shape[0]):
            hit = key[j:j + 1, :] == row
            pick = jnp.where(hit, 1.0, pick)
            gate_sel = jnp.where(hit, gate[j:j + 1, :], gate_sel)
        row1 = lax.broadcasted_iota(jnp.int32, (rows, 1), 0)
        lane = lax.broadcasted_iota(jnp.int32, ct_ref.shape[1:], 1)
        count = jnp.zeros((rows, 1), jnp.int32)
        for e in range(n_loc):
            here = jnp.sum(jnp.where(lane == me * n_loc + e, ct_ref[k], 0), axis=1, keepdims=True)
            count = jnp.where(row1 // cap == e, here, count)
        pick_ref[k] = pick.astype(BF16)
        gate_ref[k] = jnp.where(row1 % cap < count, jnp.sum(gate_sel, axis=1, keepdims=True), 0.0)

    def gated_rows(k):
        rows_k = (dot(pick_ref[k], gy_ref[k], 1, 0) * gate_ref[k]).astype(BF16)
        at = pl.multiple_of((me ^ k) * cap, cap)
        for e in range(n_loc):
            d_ref[e, pl.ds(at, cap), :] = rows_k[e * cap:(e + 1) * cap, :]

    select(0)
    gated_rows(0)
    for k in (1, 2, 3):
        for cp in small[k]:
            cp.wait()
        select(k)
    near.wait()
    gated_rows(1)
    far_head.wait_recv()
    relay_head.start()
    far_tail.wait_recv()
    gated_rows(2)
    cross_tail.wait_recv()
    relay_head.wait_recv()
    gated_rows(3)
    for cp in (far_head, far_tail, cross_tail, relay_head):
        cp.wait_send()
    for cp in loads[2:]:
        cp.wait()


def front_pass(gy, tk, sl, gt, ct, hg, hu, wd, wg, wu, n_dev, cap):
    args = (gy, tk, sl, gt, ct, hg, hu, wd, wg, wu)
    n_loc, ffn, model = wd.shape
    tok = gy.shape[0]
    rows = hg.shape[1]
    outs = [
        pltpu.VMEM((n_dev, tok, model), BF16),
        pltpu.VMEM((n_dev, n_loc * cap, tok), BF16),
        pltpu.VMEM((n_loc, rows, model), BF16),
        pltpu.VMEM((n_loc, ffn, rows), BF16),
        pltpu.VMEM((n_loc, rows, ffn), F32),
        pltpu.VMEM((n_loc, rows, ffn), F32),
        pltpu.VMEM(wd.shape, BF16),
        pltpu.VMEM((SPLIT,) + wg.shape[1:], BF16),
        pltpu.VMEM((SPLIT,) + wu.shape[1:], BF16),
    ]
    return pl.pallas_call(
        functools.partial(front_kernel, n_dev, cap),
        out_shape=outs,
        in_specs=[ANY] * len(args),
        out_specs=[VMEM] * len(outs),
        scratch_shapes=[
            pltpu.VMEM((n_dev,) + tk.shape, jnp.int32),
            pltpu.VMEM((n_dev,) + sl.shape, jnp.int32),
            pltpu.VMEM((n_dev,) + gt.shape, F32),
            pltpu.VMEM((n_dev,) + ct.shape, jnp.int32),
            pltpu.VMEM(hg.shape, BF16),
            pltpu.VMEM(hu.shape, BF16),
            pltpu.VMEM((n_dev, n_loc * cap, 1), F32),
            pltpu.SemaphoreType.DMA((5,)),
            pltpu.SemaphoreType.DMA((5,)),
            pltpu.SemaphoreType.DMA((5, n_dev)),
            pltpu.SemaphoreType.DMA((5, n_dev)),
            pltpu.SemaphoreType.DMA((4,)),
            pltpu.SemaphoreType.DMA((4,)),
        ],
        compiler_params=pltpu.CompilerParams(collective_id=0, has_side_effects=True, vmem_limit_bytes=4 * MIB),
        name="front_pass",
    )(*[pltpu.with_memory_space_constraint(a, pltpu.HBM) for a in args])


def expert_kernel(n_dev, cap, pick_ref, d_ref, act_ref, fac1_ref, fac3_ref, wd_ref, wga_ref, wua_ref, wg_in, wu_in,
                  dwd_ref, dh1_ref, dh3_ref, *rest):
    part_refs = rest[:n_dev]
    wgb_ref, wub_ref, ret_ref, stage_ref, wdt_ref, wgt_ref, wut_ref, load_sem, out_sem = rest[n_dev:]
    n_loc = wd_ref.shape[0]
    n_stage = stage_ref.shape[0]
    n_turn = wut_ref.shape[2]
    me = lax.axis_index("ep")
    loads = {e: (pltpu.make_async_copy(wg_in.at[e], wgb_ref.at[e - SPLIT], load_sem.at[0, e - SPLIT]),
                 pltpu.make_async_copy(wu_in.at[e], wub_ref.at[e - SPLIT], load_sem.at[1, e - SPLIT]))
             for e in range(SPLIT, n_loc)}
    outs = [pltpu.make_async_copy(stage_ref.at[e % n_stage], dwd_ref.at[e], out_sem.at[e % n_stage]) for e in range(n_loc)]

    def weights(e):
        return (wgb_ref[e - SPLIT], wub_ref[e - SPLIT]) if e in loads else (wga_ref[e], wua_ref[e])

    def turn_down(e):
        wdt_ref[e % 2] = wd_ref[e].T

    def turn_gate_up(e):
        wg, wu = weights(e)
        wgt_ref[e % 2] = wg.T
        wut_ref[e % 2] = wu[:n_turn].T

    def down_grad(e):
        stage_ref[e % n_stage] = dot(act_ref[e], d_ref[e], 1, 0)

    def hidden_grad(e):
        grad_h = dot(d_ref[e], wd_ref[e], 1, 1) if e == 0 else dot(d_ref[e], wdt_ref[e % 2], 1, 0)
        grad_h = grad_h.astype(BF16).astype(F32)
        dh1_ref[e] = (grad_h * fac1_ref[e]).astype(BF16)
        dh3_ref[e] = (grad_h * fac3_ref[e]).astype(BF16)

    def row_grad(e):
        wg, wu = weights(e)
        if e == 0:
            ret = dot(dh1_ref[e], wg, 1, 1) + dot(dh3_ref[e], wu, 1, 1)
        else:
            up = [dot(dh3_ref[e], wut_ref[e % 2], 1, 0), dot(dh3_ref[e], wu[n_turn:], 1, 1)]
            ret = dot(dh1_ref[e], wgt_ref[e % 2], 1, 0) + jnp.concatenate(up, axis=1)
        ret = ret.astype(BF16)
        for s in range(n_dev):
            ret_ref[s, e * cap:(e + 1) * cap, :] = ret[s * cap:(s + 1) * cap, :]

    for e in range(LEAD):
        down_grad(e)
    hidden_grad(0)
    turn_down(1)
    for e in range(0, n_loc, 2):
        for b in (e, e + 1):
            if b < n_loc and b < LEAD + e:
                outs[b].start()
        for b in (e + AHEAD, e + AHEAD + 1):
            if b in loads:
                for cp in loads[b]:
                    cp.start()
        for b in (e + LEAD, e + LEAD + 1):
            if b < n_loc and b >= n_stage:
                outs[b - n_stage].wait()
        for b in (e + 1, e + 2):
            if b in loads:
                for cp in loads[b]:
                    cp.wait()
        for f in (e, e + 1):
            if f + LEAD < n_loc:
                down_grad(f + LEAD)
            if f + 2 < n_loc:
                turn_down(f + 2)
            if f + 1 < n_loc:
                hidden_grad(f + 1)
            if f + 1 < n_loc:
                turn_gate_up(f + 1)
            row_grad(f)
    for k in range(n_dev):
        part_refs[k][...] = dot(pick_ref[k], ret_ref[me ^ k], 0, 0)
    for e in range(n_loc - n_stage, n_loc):
        outs[e].wait()


def expert_pass(pick, d, act, fac1, fac3, wd, wga, wua, wg, wu, n_dev, cap):
    n_loc, ffn, model = wd.shape
    rows = d.shape[1]
    tok = pick.shape[2]
    n_stage = 4
    late = n_loc - SPLIT
    hbm = [pltpu.with_memory_space_constraint(a, pltpu.HBM) for a in (wg, wu)]
    return pl.pallas_call(
        functools.partial(expert_kernel, n_dev, cap),
        out_shape=[
            jax.ShapeDtypeStruct((n_loc, ffn, model), F32),
            pltpu.VMEM((n_loc, rows, ffn), BF16),
            pltpu.VMEM((n_loc, rows, ffn), BF16),
        ] + [pltpu.VMEM((tok, model), F32)] * n_dev,
        in_specs=[VMEM] * 8 + [ANY] * 2,
        out_specs=[ANY, VMEM, VMEM] + [VMEM] * n_dev,
        scratch_shapes=[
            pltpu.VMEM((late,) + wg.shape[1:], BF16),
            pltpu.VMEM((late,) + wu.shape[1:], BF16),
            pltpu.VMEM((n_dev, n_loc * cap, model), BF16),
            pltpu.VMEM((n_stage, ffn, model), F32),
            pltpu.VMEM((2, model, ffn), BF16),
            pltpu.VMEM((2, ffn, model), BF16),
            pltpu.VMEM((2, ffn, model * 5 // 8), BF16),
            pltpu.SemaphoreType.DMA((2, late)),
            pltpu.SemaphoreType.DMA((n_stage,)),
        ],
        compiler_params=pltpu.CompilerParams(vmem_limit_bytes=(16 + 2 * late) * MIB + MIB // 4),
        cost_estimate=pl.CostEstimate(flops=10 * n_loc * rows * ffn * model, bytes_accessed=50 * MIB, transcendentals=0),
        name="expert_pass",
    )(pick, d, act, fac1, fac3, wd, wga, wua, *hbm)


def weight_kernel(x_ref, dh1_ref, dh3_ref, gy_ref, y_in, dwg_ref, dwu_ref, gg_ref, y_ref, stage, gg_acc, gg_out, out_sem, gg_sem):
    n_loc, _, model = x_ref.shape
    top_k = y_ref.shape[1]
    half = model // 2
    gg_copy = pltpu.make_async_copy(gg_out, gg_ref, gg_sem.at[0])
    y_copy = pltpu.make_async_copy(y_in, y_ref, gg_sem.at[1])
    y_copy.start()

    def out_copy(e, s, q):
        dst = (dwg_ref, dwu_ref)[q % 2].at[e, pl.ds(half * (q // 2), half), :]
        return pltpu.make_async_copy(stage.at[s, q], dst, out_sem.at[s, q])

    def one(e, s):
        for h in range(2):
            x = x_ref[e, :, h * half:(h + 1) * half]
            for w, dh in enumerate((dh1_ref, dh3_ref)):
                q = 2 * h + w
                stage[s, q] = dot(x, dh[e], 0, 0)
                out_copy(e, s, q).start()

    def wait_all(s):
        for q in range(4):
            out_copy(0, s, q).wait()

    def body(i, carry):
        for s in range(2):
            @pl.when(i > 0)
            def _():
                wait_all(s)
            one(2 * i + s, s)

        @pl.when(i == n_loc // 2 - 2)
        def _():
            y_copy.wait()
            step = 8
            for b in range(y_ref.shape[0] // step):
                prod = y_ref[b * step:(b + 1) * step].astype(F32) * gy_ref[0, b * step:(b + 1) * step].astype(F32)[:, None, :]
                gg_acc[b * step:(b + 1) * step, 0:top_k] = jnp.sum(prod, axis=2)
            gg_out[...] = gg_acc[...].T[0:top_k, :]
            gg_copy.start()
        return carry

    lax.fori_loop(0, n_loc // 2, body, 0)
    gg_copy.wait()
    wait_all(0)
    wait_all(1)


def weight_pass(x, dh1, dh3, gy, y):
    n_loc, rows, model = x.shape
    ffn = dh1.shape[2]
    tok, top_k, _ = y.shape
    grad_shape = jax.ShapeDtypeStruct((n_loc, model, ffn), F32)
    return pl.pallas_call(
        weight_kernel,
        out_shape=[grad_shape, grad_shape, jax.ShapeDtypeStruct((top_k, tok), F32)],
        in_specs=[VMEM] * 4 + [ANY],
        out_specs=[ANY, ANY, ANY],
        scratch_shapes=[
            pltpu.VMEM(y.shape, BF16),
            pltpu.VMEM((2, 4, model // 2, ffn), F32),
            pltpu.VMEM((tok, 128), F32),
            pltpu.VMEM((top_k, tok), F32),
            pltpu.SemaphoreType.DMA((2, 4)),
            pltpu.SemaphoreType.DMA((2,)),
        ],
        compiler_params=pltpu.CompilerParams(vmem_limit_bytes=11 * MIB),
        cost_estimate=pl.CostEstimate(flops=4 * n_loc * rows * ffn * model, bytes_accessed=40 * MIB, transcendentals=0),
        name="weight_pass",
    )(x, dh1, dh3, gy, pltpu.with_memory_space_constraint(y, pltpu.HBM))


def solution(mesh):
    n_dev = mesh.shape["ep"]
    rows_spec = P(("dp", "ep"), None)
    cube_spec = P(("dp", "ep"), None, None)
    weight_spec = P("ep", None, None)

    def local_step(grad_y, gate_vals, topk_idx, slot_ids, pair_counts, y_routed, x_disp, h_gate, h_up, w_gate, w_up, w_down):
        cap = x_disp.shape[1] // n_dev
        gy, pick, d, act, fac1, fac3, wd, wga, wua = front_pass(
            grad_y, topk_idx.T, slot_ids.T, gate_vals.T, pair_counts, h_gate, h_up, w_down, w_gate, w_up, n_dev, cap)
        dwd, dh1, dh3, *parts = expert_pass(pick, d, act, fac1, fac3, wd, wga, wua, w_gate, w_up, n_dev, cap)
        back = [lax.ppermute(parts[k], "ep", [(i, i ^ k) for i in range(n_dev)]) for k in (2, 3, 1)]
        x, _ = lax.optimization_barrier((x_disp, parts[0]))
        dwg, dwu, gg = weight_pass(x, dh1, dh3, gy, y_routed)
        total = parts[0]
        for b in back:
            total = total + b
        return total.astype(BF16), gg.T, dwg, dwu, dwd

    return jax.shard_map(local_step, mesh=mesh, in_specs=(rows_spec, rows_spec, rows_spec, rows_spec, rows_spec, cube_spec, cube_spec, cube_spec, cube_spec, weight_spec, weight_spec, weight_spec), out_specs=(rows_spec, rows_spec, cube_spec, cube_spec, cube_spec), check_vma=False)
```

```python
import functools

import jax
import jax.numpy as jnp
from jax import lax
from jax.experimental import pallas as pl
from jax.experimental.pallas import tpu as pltpu
from jax.sharding import PartitionSpec as P

MESH = pl.DeviceIdType.MESH
F32 = jnp.float32
BF16 = jnp.bfloat16
ANY = pl.BlockSpec(memory_space=pl.ANY)
VMEM = pl.BlockSpec(memory_space=pltpu.VMEM)
MIB = 2**20
SPLIT = 6
AHEAD = 4
DIRECT = 16
LEAD = 2


def dot(a, b, ca, cb):
    return lax.dot_general(a, b, (((ca,), (cb,)), ((), ())), preferred_element_type=F32)


def front_kernel(n_dev, cap, gy_in, tk_in, sl_in, gt_in, ct_in, hg_in, hu_in, wd_in, wg_in, wu_in,
                 gy_ref, pick_ref, d_ref, act_ref, fac1_ref, fac3_ref, wd_ref, wg_ref, wu_ref,
                 tk_ref, sl_ref, gt_ref, ct_ref, hg_ref, hu_ref, gate_ref, local_sem, load_sem, send_sem, recv_sem, piece_send, piece_recv):
    me = lax.axis_index("ep")
    n_loc = d_ref.shape[0]
    bufs = [gy_ref, tk_ref, sl_ref, gt_ref, ct_ref]
    ins = [gy_in, tk_in, sl_in, gt_in, ct_in]
    local = [pltpu.make_async_copy(a, b.at[0], local_sem.at[i])
             for i, (a, b) in enumerate(zip((gy_in, tk_in, sl_in, gt_in, ct_in), bufs))]
    pairs = [(hg_in, hg_ref), (hu_in, hu_ref), (wd_in, wd_ref), (wg_in.at[pl.ds(0, SPLIT)], wg_ref),
             (wu_in.at[pl.ds(0, SPLIT)], wu_ref)]
    loads = [pltpu.make_async_copy(a, b, load_sem.at[i]) for i, (a, b) in enumerate(pairs)]
    for cp in local:
        cp.start()
    barrier = pltpu.get_barrier_semaphore()
    for k in range(1, n_dev):
        pl.semaphore_signal(barrier, inc=1, device_id={"ep": me ^ k}, device_id_type=MESH)
    for cp in loads:
        cp.start()
    pl.semaphore_wait(barrier, n_dev - 1)

    def remote(i, k):
        return pltpu.make_async_remote_copy(
            src_ref=ins[i], dst_ref=bufs[i].at[k], send_sem=send_sem.at[i, k], recv_sem=recv_sem.at[i, k],
            device_id={"ep": me ^ k}, device_id_type=MESH)

    def piece(n, k, src, slot, at, size):
        return pltpu.make_async_remote_copy(
            src_ref=src.at[pl.ds(at, size)], dst_ref=gy_ref.at[slot, pl.ds(at, size)],
            send_sem=piece_send.at[n], recv_sem=piece_recv.at[n], device_id={"ep": me ^ k}, device_id_type=MESH)

    tok = gy_in.shape[0]
    head = tok - DIRECT
    far_head = piece(0, 2, gy_in, 2, 0, head)
    far_tail = piece(1, 2, gy_in, 2, head, DIRECT)
    cross_tail = piece(2, 3, gy_in, 3, head, DIRECT)
    relay_head = piece(3, 1, gy_ref.at[2], 3, 0, head)
    near = remote(0, 1)
    small = {k: [remote(i, k) for i in range(1, len(bufs))] for k in range(1, n_dev)}
    for k in (2, 3):
        for cp in small[k]:
            cp.start()
    far_head.start()
    far_tail.start()
    cross_tail.start()
    for cp in small[1]:
        cp.start()
    near.start()

    for cp in local:
        cp.wait()
    loads[0].wait()
    loads[1].wait()

    def silu(e, carry):
        gate_f = hg_ref[e].astype(F32)
        up_f = hu_ref[e].astype(F32)
        gate_sig = jax.nn.sigmoid(gate_f)
        gate_act = gate_f * gate_sig
        act_ref[e] = (gate_act * up_f).astype(BF16).T
        fac1_ref[e] = up_f * gate_sig * (1.0 + gate_f * (1.0 - gate_sig))
        fac3_ref[e] = gate_act
        return carry

    lax.fori_loop(0, n_loc, silu, 0)

    rows = n_loc * cap

    def select(k):
        row = lax.broadcasted_iota(jnp.int32, (rows, tok), 0) + me * rows
        key = jnp.where(sl_ref[k] >= 0, tk_ref[k] * cap + sl_ref[k], -1)
        gate = gt_ref[k]
        pick = jnp.zeros((rows, tok), F32)
        gate_sel = jnp.zeros((rows, tok), F32)
        for j in range(key.shape[0]):
            hit = key[j:j + 1, :] == row
            pick = jnp.where(hit, 1.0, pick)
            gate_sel = jnp.where(hit, gate[j:j + 1, :], gate_sel)
        row1 = lax.broadcasted_iota(jnp.int32, (rows, 1), 0)
        lane = lax.broadcasted_iota(jnp.int32, ct_ref.shape[1:], 1)
        count = jnp.zeros((rows, 1), jnp.int32)
        for e in range(n_loc):
            here = jnp.sum(jnp.where(lane == me * n_loc + e, ct_ref[k], 0), axis=1, keepdims=True)
            count = jnp.where(row1 // cap == e, here, count)
        pick_ref[k] = pick.astype(BF16)
        gate_ref[k] = jnp.where(row1 % cap < count, jnp.sum(gate_sel, axis=1, keepdims=True), 0.0)

    def gated_rows(k):
        rows_k = (dot(pick_ref[k], gy_ref[k], 1, 0) * gate_ref[k]).astype(BF16)
        at = pl.multiple_of((me ^ k) * cap, cap)
        for e in range(n_loc):
            d_ref[e, pl.ds(at, cap), :] = rows_k[e * cap:(e + 1) * cap, :]

    select(0)
    gated_rows(0)
    for k in (1, 2, 3):
        for cp in small[k]:
            cp.wait()
        select(k)
    near.wait()
    gated_rows(1)
    far_head.wait_recv()
    relay_head.start()
    far_tail.wait_recv()
    gated_rows(2)
    cross_tail.wait_recv()
    relay_head.wait_recv()
    gated_rows(3)
    for cp in (far_head, far_tail, cross_tail, relay_head):
        cp.wait_send()
    for cp in loads[2:]:
        cp.wait()


def front_pass(gy, tk, sl, gt, ct, hg, hu, wd, wg, wu, n_dev, cap):
    args = (gy, tk, sl, gt, ct, hg, hu, wd, wg, wu)
    n_loc, ffn, model = wd.shape
    tok = gy.shape[0]
    rows = hg.shape[1]
    outs = [
        pltpu.VMEM((n_dev, tok, model), BF16),
        pltpu.VMEM((n_dev, n_loc * cap, tok), BF16),
        pltpu.VMEM((n_loc, rows, model), BF16),
        pltpu.VMEM((n_loc, ffn, rows), BF16),
        pltpu.VMEM((n_loc, rows, ffn), F32),
        pltpu.VMEM((n_loc, rows, ffn), F32),
        pltpu.VMEM(wd.shape, BF16),
        pltpu.VMEM((SPLIT,) + wg.shape[1:], BF16),
        pltpu.VMEM((SPLIT,) + wu.shape[1:], BF16),
    ]
    return pl.pallas_call(
        functools.partial(front_kernel, n_dev, cap),
        out_shape=outs,
        in_specs=[ANY] * len(args),
        out_specs=[VMEM] * len(outs),
        scratch_shapes=[
            pltpu.VMEM((n_dev,) + tk.shape, jnp.int32),
            pltpu.VMEM((n_dev,) + sl.shape, jnp.int32),
            pltpu.VMEM((n_dev,) + gt.shape, F32),
            pltpu.VMEM((n_dev,) + ct.shape, jnp.int32),
            pltpu.VMEM(hg.shape, BF16),
            pltpu.VMEM(hu.shape, BF16),
            pltpu.VMEM((n_dev, n_loc * cap, 1), F32),
            pltpu.SemaphoreType.DMA((5,)),
            pltpu.SemaphoreType.DMA((5,)),
            pltpu.SemaphoreType.DMA((5, n_dev)),
            pltpu.SemaphoreType.DMA((5, n_dev)),
            pltpu.SemaphoreType.DMA((4,)),
            pltpu.SemaphoreType.DMA((4,)),
        ],
        compiler_params=pltpu.CompilerParams(collective_id=0, has_side_effects=True, vmem_limit_bytes=4 * MIB),
        name="front_pass",
    )(*[pltpu.with_memory_space_constraint(a, pltpu.HBM) for a in args])


def expert_kernel(n_dev, cap, pick_ref, d_ref, act_ref, fac1_ref, fac3_ref, wd_ref, wga_ref, wua_ref, wg_in, wu_in,
                  dwd_ref, dh1_ref, dh3_ref, *rest):
    part_refs = rest[:n_dev]
    wgb_ref, wub_ref, ret_ref, stage_ref, wdt_ref, wgt_ref, wut_ref, load_sem, out_sem = rest[n_dev:]
    n_loc = wd_ref.shape[0]
    n_stage = stage_ref.shape[0]
    n_turn = wut_ref.shape[2]
    me = lax.axis_index("ep")
    loads = {e: (pltpu.make_async_copy(wg_in.at[e], wgb_ref.at[e - SPLIT], load_sem.at[0, e - SPLIT]),
                 pltpu.make_async_copy(wu_in.at[e], wub_ref.at[e - SPLIT], load_sem.at[1, e - SPLIT]))
             for e in range(SPLIT, n_loc)}
    outs = [pltpu.make_async_copy(stage_ref.at[e % n_stage], dwd_ref.at[e], out_sem.at[e % n_stage]) for e in range(n_loc)]

    def weights(e):
        return (wgb_ref[e - SPLIT], wub_ref[e - SPLIT]) if e in loads else (wga_ref[e], wua_ref[e])

    def turn_down(e):
        wdt_ref[e % 2] = wd_ref[e].T

    def turn_gate_up(e):
        wg, wu = weights(e)
        wgt_ref[e % 2] = wg.T
        wut_ref[e % 2] = wu[:n_turn].T

    def down_grad(e):
        stage_ref[e % n_stage] = dot(act_ref[e], d_ref[e], 1, 0)

    def hidden_grad(e):
        grad_h = dot(d_ref[e], wd_ref[e], 1, 1) if e == 0 else dot(d_ref[e], wdt_ref[e % 2], 1, 0)
        grad_h = grad_h.astype(BF16).astype(F32)
        dh1_ref[e] = (grad_h * fac1_ref[e]).astype(BF16)
        dh3_ref[e] = (grad_h * fac3_ref[e]).astype(BF16)

    def row_grad(e):
        wg, wu = weights(e)
        if e == 0:
            ret = dot(dh1_ref[e], wg, 1, 1) + dot(dh3_ref[e], wu, 1, 1)
        else:
            up = [dot(dh3_ref[e], wut_ref[e % 2], 1, 0), dot(dh3_ref[e], wu[n_turn:], 1, 1)]
            ret = dot(dh1_ref[e], wgt_ref[e % 2], 1, 0) + jnp.concatenate(up, axis=1)
        ret = ret.astype(BF16)
        for s in range(n_dev):
            ret_ref[s, e * cap:(e + 1) * cap, :] = ret[s * cap:(s + 1) * cap, :]

    for e in range(LEAD):
        down_grad(e)
    hidden_grad(0)
    turn_down(1)
    for e in range(0, n_loc, 2):
        for b in (e, e + 1):
            if b < n_loc and b < LEAD + e:
                outs[b].start()
        for b in (e + AHEAD, e + AHEAD + 1):
            if b in loads:
                for cp in loads[b]:
                    cp.start()
        for b in (e + LEAD, e + LEAD + 1):
            if b < n_loc and b >= n_stage:
                outs[b - n_stage].wait()
        for b in (e + 1, e + 2):
            if b in loads:
                for cp in loads[b]:
                    cp.wait()
        for f in (e, e + 1):
            if f + 2 < n_loc:
                turn_down(f + 2)
            if f + LEAD < n_loc:
                down_grad(f + LEAD)
            if f + 1 < n_loc:
                hidden_grad(f + 1)
            if f + 1 < n_loc:
                turn_gate_up(f + 1)
            row_grad(f)
    for k in range(n_dev):
        part_refs[k][...] = dot(pick_ref[k], ret_ref[me ^ k], 0, 0)
    for e in range(n_loc - n_stage, n_loc):
        outs[e].wait()


def expert_pass(pick, d, act, fac1, fac3, wd, wga, wua, wg, wu, n_dev, cap):
    n_loc, ffn, model = wd.shape
    rows = d.shape[1]
    tok = pick.shape[2]
    n_stage = 4
    late = n_loc - SPLIT
    hbm = [pltpu.with_memory_space_constraint(a, pltpu.HBM) for a in (wg, wu)]
    return pl.pallas_call(
        functools.partial(expert_kernel, n_dev, cap),
        out_shape=[
            jax.ShapeDtypeStruct((n_loc, ffn, model), F32),
            pltpu.VMEM((n_loc, rows, ffn), BF16),
            pltpu.VMEM((n_loc, rows, ffn), BF16),
        ] + [pltpu.VMEM((tok, model), F32)] * n_dev,
        in_specs=[VMEM] * 8 + [ANY] * 2,
        out_specs=[ANY, VMEM, VMEM] + [VMEM] * n_dev,
        scratch_shapes=[
            pltpu.VMEM((late,) + wg.shape[1:], BF16),
            pltpu.VMEM((late,) + wu.shape[1:], BF16),
            pltpu.VMEM((n_dev, n_loc * cap, model), BF16),
            pltpu.VMEM((n_stage, ffn, model), F32),
            pltpu.VMEM((2, model, ffn), BF16),
            pltpu.VMEM((2, ffn, model), BF16),
            pltpu.VMEM((2, ffn, model * 5 // 8), BF16),
            pltpu.SemaphoreType.DMA((2, late)),
            pltpu.SemaphoreType.DMA((n_stage,)),
        ],
        compiler_params=pltpu.CompilerParams(vmem_limit_bytes=(16 + 2 * late) * MIB + MIB // 4),
        cost_estimate=pl.CostEstimate(flops=10 * n_loc * rows * ffn * model, bytes_accessed=50 * MIB, transcendentals=0),
        name="expert_pass",
    )(pick, d, act, fac1, fac3, wd, wga, wua, *hbm)


def weight_kernel(x_ref, dh1_ref, dh3_ref, gy_ref, y_in, dwg_ref, dwu_ref, gg_ref, y_ref, stage, gg_acc, gg_out, out_sem, gg_sem):
    n_loc, _, model = x_ref.shape
    top_k = y_ref.shape[1]
    half = model // 2
    gg_copy = pltpu.make_async_copy(gg_out, gg_ref, gg_sem.at[0])
    y_copy = pltpu.make_async_copy(y_in, y_ref, gg_sem.at[1])
    y_copy.start()

    def out_copy(e, s, q):
        dst = (dwg_ref, dwu_ref)[q % 2].at[e, pl.ds(half * (q // 2), half), :]
        return pltpu.make_async_copy(stage.at[s, q], dst, out_sem.at[s, q])

    def one(e, s):
        for h in range(2):
            x = x_ref[e, :, h * half:(h + 1) * half]
            for w, dh in enumerate((dh1_ref, dh3_ref)):
                q = 2 * h + w
                stage[s, q] = dot(x, dh[e], 0, 0)
                out_copy(e, s, q).start()

    def wait_all(s):
        for q in range(4):
            out_copy(0, s, q).wait()

    def body(i, carry):
        for s in range(2):
            @pl.when(i > 0)
            def _():
                wait_all(s)
            one(2 * i + s, s)

        @pl.when(i == n_loc // 2 - 2)
        def _():
            y_copy.wait()
            step = 8
            for b in range(y_ref.shape[0] // step):
                prod = y_ref[b * step:(b + 1) * step].astype(F32) * gy_ref[0, b * step:(b + 1) * step].astype(F32)[:, None, :]
                gg_acc[b * step:(b + 1) * step, 0:top_k] = jnp.sum(prod, axis=2)
            gg_out[...] = gg_acc[...].T[0:top_k, :]
            gg_copy.start()
        return carry

    lax.fori_loop(0, n_loc // 2, body, 0)
    gg_copy.wait()
    wait_all(0)
    wait_all(1)


def weight_pass(x, dh1, dh3, gy, y):
    n_loc, rows, model = x.shape
    ffn = dh1.shape[2]
    tok, top_k, _ = y.shape
    grad_shape = jax.ShapeDtypeStruct((n_loc, model, ffn), F32)
    return pl.pallas_call(
        weight_kernel,
        out_shape=[grad_shape, grad_shape, jax.ShapeDtypeStruct((top_k, tok), F32)],
        in_specs=[VMEM] * 4 + [ANY],
        out_specs=[ANY, ANY, ANY],
        scratch_shapes=[
            pltpu.VMEM(y.shape, BF16),
            pltpu.VMEM((2, 4, model // 2, ffn), F32),
            pltpu.VMEM((tok, 128), F32),
            pltpu.VMEM((top_k, tok), F32),
            pltpu.SemaphoreType.DMA((2, 4)),
            pltpu.SemaphoreType.DMA((2,)),
        ],
        compiler_params=pltpu.CompilerParams(vmem_limit_bytes=11 * MIB),
        cost_estimate=pl.CostEstimate(flops=4 * n_loc * rows * ffn * model, bytes_accessed=40 * MIB, transcendentals=0),
        name="weight_pass",
    )(x, dh1, dh3, gy, pltpu.with_memory_space_constraint(y, pltpu.HBM))


def solution(mesh):
    n_dev = mesh.shape["ep"]
    rows_spec = P(("dp", "ep"), None)
    cube_spec = P(("dp", "ep"), None, None)
    weight_spec = P("ep", None, None)

    def local_step(grad_y, gate_vals, topk_idx, slot_ids, pair_counts, y_routed, x_disp, h_gate, h_up, w_gate, w_up, w_down):
        cap = x_disp.shape[1] // n_dev
        gy, pick, d, act, fac1, fac3, wd, wga, wua = front_pass(
            grad_y, topk_idx.T, slot_ids.T, gate_vals.T, pair_counts, h_gate, h_up, w_down, w_gate, w_up, n_dev, cap)
        dwd, dh1, dh3, *parts = expert_pass(pick, d, act, fac1, fac3, wd, wga, wua, w_gate, w_up, n_dev, cap)
        back = [lax.ppermute(parts[k], "ep", [(i, i ^ k) for i in range(n_dev)]) for k in (2, 3, 1)]
        x, _ = lax.optimization_barrier((x_disp, parts[0]))
        dwg, dwu, gg = weight_pass(x, dh1, dh3, gy, y_routed)
        total = parts[0]
        for b in back:
            total = total + b
        return total.astype(BF16), gg.T, dwg, dwu, dwd

    return jax.shard_map(local_step, mesh=mesh, in_specs=(rows_spec, rows_spec, rows_spec, rows_spec, rows_spec, cube_spec, cube_spec, cube_spec, cube_spec, weight_spec, weight_spec, weight_spec), out_specs=(rows_spec, rows_spec, cube_spec, cube_spec, cube_spec), check_vma=False)
```
